32 devices in a mesh: freq: 8 (over z, core), rows: 4 (over y, x).
Axes of the slice: x: 2, y: 2, z: 4, core: 2. Of those that a mesh axis runs over, the one named last changes fastest.
Arguments:
- wavefield: float32 [2, 8, 1024, 2048], P(None, 'freq', 'rows'), may hold values from -28 to 28
- block_inverse: bfloat16 [2, 8, 16, 128, 128], P(None, 'freq'), may hold values from -0.19921875 to 0.19921875
- coefficient: bfloat16 [1024, 2048], P('rows'), may hold values from 0.049804688 to 0.29882812
- correction_factor: float32 [2, 8], P(None, 'freq'), may hold values from -4 to 4
- frequencies: float32 [8], P('freq'), may hold values from 1.5 to 4.5
- slowness: float32 [2], replicated, may hold values from 0.7 to 1
Outputs:
- depth_image: float32 [2, 1024, 2048], P(None, 'rows', 'freq')
- final_field: float32 [2, 8, 1024, 2048], P(None, 'freq', 'rows')
The draws below stay inside these ranges and needn't reach their ends.
All inputs are finite; a program needn't handle non-finite values.
Results may differ from the reference program's by a relative error of at most 0.023.
Values may be sent and summed in bfloat16 or wider, within the bound.
No kernel may reach another device: no remote copies, remote signals or barrier semaphores. Data moves between devices by JAX's collectives and lax.ppermute only.
A program may use at most 64 MiB of HBM per device.

```python
import math
import jax
import jax.numpy as jnp
from jax import lax

NX = 2048
NY = 1024
BLOCK = 128
DEPTHS = 2
NW = 8


def draw_wavefield(key, part):
    noise_key = jax.random.fold_in(key, 11)
    column_key = jax.random.fold_in(key, 12)
    common_key = jax.random.fold_in(key, 13)
    region_key = jax.random.fold_in(key, 14)
    position = jnp.arange(NY, dtype=jnp.float32) / max(NY - 1, 1)
    column_scale = 10.0 ** jax.random.uniform(column_key, (NX,), jnp.float32)
    region_pick = jax.random.randint(region_key, (4, 16), 0, 10)
    region_weight = jnp.where(region_pick < 3, 0.95, 0.15).astype(jnp.float32)
    row_quarter = jnp.arange(NY, dtype=jnp.int32) * 4 // NY
    column_block = jnp.arange(NX, dtype=jnp.int32) * 16 // NX
    shared_weight = region_weight[row_quarter][:, column_block]
    own_weight = jnp.sqrt(1.0 - shared_weight * shared_weight)
    base_noise = jnp.clip(jax.random.normal(noise_key, (2, NW, NY, NX), jnp.float32), -6.0, 6.0)
    common_noise = jnp.clip(jax.random.normal(common_key, (2, 1, NY, NX), jnp.float32), -6.0, 6.0)
    base_noise = jnp.clip(own_weight * base_noise + shared_weight * common_noise, -6.0, 6.0)
    row_scale = 10.0 ** position
    return base_noise * (row_scale[:, None] * column_scale[None, :]) / 21.5


def block_levels(rng, extent, pieces, low, largest):
    factor_of, own = 1.0, jax.random.fold_in(rng, 6)
    for dim, blocks in pieces:
        steps = jnp.exp(jax.random.uniform(jax.random.fold_in(own, dim), (blocks,), jnp.float32, low / len(pieces), largest / len(pieces)))
        factor_of = factor_of * jnp.repeat(steps, extent[dim] // blocks).reshape([-1 if axis == dim else 1 for axis in range(len(extent))])
    return factor_of


def centred(key, dims, deviation, bound, cuts=(), kind=jnp.bfloat16):
    gain = block_levels(key, dims, cuts, -0.22, 0.18) if cuts else 1.0
    values = jax.random.normal(key, dims, jnp.float32) * deviation * gain
    return jnp.minimum(jnp.maximum(values, -bound), bound).astype(kind)


def setup_inputs(seed: int = 0) -> dict:
    splits = jax.random.split(jax.random.key(seed), 7)
    return {
        "wavefield": draw_wavefield(jax.random.fold_in(splits[6], 71), 0),
        "block_inverse": centred(splits[1], (2, NW, NX // BLOCK, BLOCK, BLOCK), 0.03, 0.19921875, ((1, 8),)),
        "coefficient": jnp.clip(jnp.exp(math.log(0.29882812) - 1.7917595 * jax.random.uniform(splits[2], (NY, NX), jnp.float32) ** block_levels(splits[2], (NY, NX), ((0, 4),), -0.2, 0.2)), 0.049804688, 0.29882812).astype(jnp.bfloat16),
        "correction_factor": centred(splits[3], (2, NW), 1.0, 4.0, ((1, 8),), jnp.float32),
        "frequencies": jnp.clip(1.5 + 3.0 * jax.random.uniform(splits[4], (NW,), jnp.float32) ** block_levels(splits[4], (NW,), ((0, 8),), -0.2, 0.2), 1.5, 4.5),
        "slowness": jnp.clip(jax.random.uniform(splits[5], (DEPTHS,), jnp.float32, 0.7, 1.0), 0.7, 1.0),
    }


def wavenumbers(length, offset, count):
    indices = offset + jnp.arange(count, dtype=jnp.int32)
    signed = jnp.where(2 * indices < length, indices, indices - length)
    return signed.astype(jnp.float32) * (2.0 * jnp.pi / length)

def to_bfloat(values):
    return lax.optimization_barrier(values.astype(jnp.bfloat16)).astype(jnp.float32)

def blockwise(left_rows, right_blocks):
    return jnp.einsum('ybi,bij->ybj', left_rows, right_blocks, precision=lax.Precision.HIGHEST)

def reference(wavefield, block_inverse, coefficient, correction_factor, frequencies, slowness):
    kappa_y = wavenumbers(NY, 0, NY)
    kappa_x = wavenumbers(NX, 0, NX)
    coef_full = coefficient.astype(jnp.float32)
    block_count = NX // BLOCK

    def one_frequency(image_sums, freq_index):
        field_pair = lax.dynamic_index_in_dim(wavefield, freq_index, 1, keepdims=False)
        block_pair = lax.dynamic_index_in_dim(block_inverse, freq_index, 1, keepdims=False).astype(jnp.float32)
        factor_pair = lax.dynamic_index_in_dim(correction_factor, freq_index, 1, keepdims=False)
        omega_value = lax.dynamic_index_in_dim(frequencies, freq_index, 0, keepdims=False)
        real_part = field_pair[0]
        imag_part = field_pair[1]
        for depth_step in range(DEPTHS):
            spectrum = jnp.fft.fft(real_part + 1j * imag_part, axis=1)
            spectrum = to_bfloat(spectrum.real) + 1j * to_bfloat(spectrum.imag)
            spectrum = jnp.fft.fft(spectrum, axis=0)
            vertical = (omega_value * slowness[depth_step]) ** 2 - kappa_y[:, None] ** 2 - kappa_x[None, :] ** 2
            root_value = jnp.sqrt(jnp.abs(vertical))
            upward = vertical >= 0.0
            prop_real = jnp.where(upward, jnp.cos(root_value), jnp.exp(-root_value))
            prop_imag = jnp.where(upward, jnp.sin(root_value), 0.0)
            spectrum = spectrum * (prop_real + 1j * prop_imag)
            returned = jnp.fft.ifft(spectrum, axis=0)
            returned = to_bfloat(returned.real) + 1j * to_bfloat(returned.imag)
            space_field = jnp.fft.ifft(returned, axis=1)
            space_real = space_field.real
            space_imag = space_field.imag
            padded_real = jnp.pad(space_real, ((1, 1), (0, 0)))
            padded_imag = jnp.pad(space_imag, ((1, 1), (0, 0)))
            curve_real = padded_real[2:] - 2.0 * space_real + padded_real[:-2]
            curve_imag = padded_imag[2:] - 2.0 * space_imag + padded_imag[:-2]
            corrected_real = space_real + coef_full * (factor_pair[0] * curve_real - factor_pair[1] * curve_imag)
            corrected_imag = space_imag + coef_full * (factor_pair[0] * curve_imag + factor_pair[1] * curve_real)
            rounded_real = to_bfloat(corrected_real).reshape(NY, block_count, BLOCK)
            rounded_imag = to_bfloat(corrected_imag).reshape(NY, block_count, BLOCK)
            new_real = corrected_real + (blockwise(rounded_real, block_pair[0]) - blockwise(rounded_imag, block_pair[1])).reshape(NY, NX)
            new_imag = corrected_imag + (blockwise(rounded_real, block_pair[1]) + blockwise(rounded_imag, block_pair[0])).reshape(NY, NX)
            image_sums = image_sums.at[depth_step].add(new_real)
            real_part = new_real
            imag_part = new_imag
        return (image_sums, jnp.stack([real_part, imag_part]))
    start_sums = jnp.zeros((DEPTHS, NY, NX), jnp.float32)
    image_sums, finals = lax.scan(one_frequency, start_sums, jnp.arange(NW, dtype=jnp.int32))
    energy = lax.optimization_barrier(jnp.mean(image_sums * image_sums, axis=(1, 2), keepdims=True))
    depth_image = image_sums / jnp.sqrt(energy + 1e-06)
    return (depth_image, jnp.moveaxis(finals, 0, 1))
```

```python
import functools
import math

import jax
import jax.numpy as jnp
import numpy as np
from jax import lax
from jax.experimental import pallas as pl
from jax.experimental.pallas import tpu as pltpu
from jax.sharding import PartitionSpec as P

DEPTHS = 2
epsilon = 1e-06
F32 = jnp.float32
BF16 = jnp.bfloat16
VMEM_LIMIT = 36 * 1024 * 1024
EXTRA = 16


def small_dft(real, imag, sign):
    count = len(real)
    if count == 1:
        return list(real), list(imag)
    even_r, even_i = small_dft(real[0::2], imag[0::2], sign)
    odd_r, odd_i = small_dft(real[1::2], imag[1::2], sign)
    half = count // 2
    out_r, out_i = [None] * count, [None] * count
    for k in range(half):
        br, bi = odd_r[k], odd_i[k]
        if k == 0:
            tr, ti = br, bi
        elif 4 * k == count:
            tr, ti = (-bi, br) if sign > 0 else (bi, -br)
            if sign > 0:
                out_r[k], out_i[k] = even_r[k] - bi, even_i[k] + br
                out_r[k + half], out_i[k + half] = even_r[k] + bi, even_i[k] - br
            else:
                out_r[k], out_i[k] = even_r[k] + bi, even_i[k] - br
                out_r[k + half], out_i[k + half] = even_r[k] - bi, even_i[k] + br
            continue
        else:
            angle = sign * 2.0 * math.pi * k / count
            c, s = math.cos(angle), math.sin(angle)
            if abs(abs(c) - abs(s)) < 1e-12:
                h = abs(c)
                cs, ss = math.copysign(1.0, c), math.copysign(1.0, s)
                re = (br if cs > 0 else -br) + (-bi if ss > 0 else bi)
                im = (bi if cs > 0 else -bi) + (br if ss > 0 else -br)
                tr, ti = re * h, im * h
            else:
                tr, ti = br * c - bi * s, br * s + bi * c
        out_r[k], out_i[k] = even_r[k] + tr, even_i[k] + ti
        out_r[k + half], out_i[k + half] = even_r[k] - tr, even_i[k] - ti
    return out_r, out_i


def lane_tables(width, lane):
    blocks = width // lane
    a = np.arange(lane)
    forward = np.exp(-2j * np.pi * np.outer(a, a) / lane)
    inverse = np.exp(2j * np.pi * np.outer(a, a) / lane) / width

    def embed(m):
        return np.block([[m.real, m.imag], [-m.imag, m.real]])

    twist = np.exp(-2j * np.pi * np.outer(np.arange(blocks), a) / width)
    return (
        jnp.asarray(embed(forward), BF16),
        jnp.asarray(embed(inverse), BF16),
        jnp.asarray(np.stack([twist.real, twist.imag]), F32),
    )


def row_tables(height, lane):
    count = height // lane
    a = np.arange(lane)
    forward, inverse = [], []
    for k in range(count):
        j = a if 2 * k <= count else lane - 1 - a
        ky = count * j + k
        table = np.exp(-2j * np.pi * np.outer(ky, a) / height)
        forward.append(np.block([[table.real, -table.imag], [table.imag, table.real]]))
        back = np.conj(table.T) / height
        inverse.append(np.block([[back.real, -back.imag], [back.imag, back.real]]))
    return jnp.asarray(np.stack(forward), BF16), jnp.asarray(np.stack(inverse), BF16)


def dot(left, right):
    return jnp.dot(left, right, preferred_element_type=F32)

ANY = pl.BlockSpec(memory_space=pltpu.HBM)
SMEM = pl.BlockSpec(memory_space=pltpu.SMEM)
FULL = pl.BlockSpec(memory_space=pltpu.VMEM)


def cost(flops, moved):
    return pl.CostEstimate(flops=flops, bytes_accessed=moved, transcendentals=0)


def params():
    return pltpu.CompilerParams(vmem_limit_bytes=VMEM_LIMIT)


def forward_lanes(load, rows, blocks, lane, twist_ref, left_ref, base=0):
    sub = 16

    def body(i, carry):
        at = pl.ds(pl.multiple_of(i * sub, sub), sub)
        to = pl.ds(pl.multiple_of(i * sub + base, sub), sub)
        real = [load(0, at, b) for b in range(blocks)]
        imag = [load(1, at, b) for b in range(blocks)]
        real, imag = small_dft(real, imag, -1)
        for k in range(blocks):
            if k:
                c, s = twist_ref[0, k : k + 1, :], twist_ref[1, k : k + 1, :]
                re, im = real[k] * c - imag[k] * s, real[k] * s + imag[k] * c
            else:
                re, im = real[k], imag[k]
            left_ref[k, to, 0:lane] = re.astype(BF16)
            left_ref[k, to, lane : 2 * lane] = im.astype(BF16)
        return carry

    lax.fori_loop(0, rows // sub, body, 0)


def slot_products(left_ref, table_ref, me, slot, per_device):
    owner = lax.bitwise_xor(me, slot)
    left = left_ref[pl.ds(owner * per_device, per_device)]
    count, rows, wide = left.shape
    part = dot(left.reshape(count * rows, wide), table_ref[...]).astype(BF16)
    return [part[place * rows : (place + 1) * rows] for place in range(per_device)]


def first_kernel(me_ref, field_hbm, twist_ref, table_ref, *refs, lane, per_device, chunk, parts):
    outs, (field_ref, left_ref, sem) = refs[:-3], refs[-3:]
    rows, width = field_ref.shape[1], field_ref.shape[2]
    tile = rows // parts
    arriving = [
        pltpu.make_async_copy(
            field_hbm.at[:, pl.ds(chunk * rows + t * tile, tile), :],
            field_ref.at[:, pl.ds(t * tile, tile), :],
            sem.at[t],
        )
        for t in range(parts)
    ]
    for copy in arriving:
        copy.start()
    for t in range(parts):
        arriving[t].wait()

        def load(part, at, b, t=t):
            return field_ref[part, pl.ds(at.start + t * tile, at.size), b * lane : (b + 1) * lane]

        forward_lanes(load, tile, width // lane, lane, twist_ref, left_ref, t * tile)
    for slot, out_ref in enumerate(outs):
        made = slot_products(left_ref, table_ref, me_ref[0], slot, per_device)
        for place, part in enumerate(made):
            out_ref[:, place * 2 * lane : (place + 1) * 2 * lane] = part


def forward_x(me, field, tables, lane, devices, chunk, chunks):
    _, rows, width = field.shape
    blocks = width // lane
    per_device = blocks // devices
    rows = rows // chunks
    parts = max(rows // 32, 1)
    wide = per_device * 2 * lane
    return pl.pallas_call(
        functools.partial(
            first_kernel, lane=lane, per_device=per_device, chunk=chunk, parts=parts
        ),
        in_specs=[SMEM, ANY, FULL, FULL],
        out_specs=[FULL] * devices,
        out_shape=[jax.ShapeDtypeStruct((rows, wide), BF16)] * devices,
        scratch_shapes=[
            pltpu.VMEM((2, rows, width), F32),
            pltpu.VMEM((blocks, rows, 2 * lane), BF16),
            pltpu.SemaphoreType.DMA((parts,)),
        ],
        compiler_params=params(),
        cost_estimate=cost(rows * width * 4000, rows * width * 12),
        name="forward_x",
    )(me, field, tables[2], tables[0])


def poly(coefficients, t):
    acc = jnp.full_like(t, coefficients[-1])
    for c in coefficients[-2::-1]:
        acc = acc * t + c
    return acc


@functools.lru_cache(maxsize=None)
def wave_series(limit):
    from numpy.polynomial import chebyshev

    nodes = np.cos(np.pi * (np.arange(64) + 0.5) / 64)
    root = np.sqrt((nodes + 1.0) * 0.5 * limit)
    out = []
    for values in (np.cos(root), np.sinc(root / np.pi)):
        fitted = chebyshev.chebfit(nodes, values, 7)
        out.append(tuple(float(c) for c in chebyshev.cheb2poly(fitted)))
    return tuple(out)


def propagator(q, limit):
    root = jnp.sqrt(jnp.abs(q))
    t = q * (2.0 / limit) - 1.0
    cosine, sinc = wave_series(limit)
    upward = q >= 0.0
    t = jnp.where(upward, t, 0.0)
    real = jnp.where(upward, poly(cosine, t), jnp.exp(-root))
    imag = jnp.where(upward, root * poly(sinc, t), 0.0)
    return real, imag


def wave_kernel(me_ref, squared_ref, after_ref, *u_refs, lane, width, height, columns, limit):
    me = me_ref[0]
    depths = len(u_refs)
    count = height // lane
    blocks = width // lane
    sub = 8
    col = lax.broadcasted_iota(jnp.int32, (sub, lane), 1)
    row_id = lax.broadcasted_iota(jnp.int32, (sub, lane), 0)

    def kappa_squared(index, length):
        signed = jnp.where(2 * index < length, index, index - length)
        kappa = signed.astype(F32) * (2.0 * math.pi / length)
        return kappa * kappa

    def wave_body(i, carry):
        at = pl.multiple_of(i * sub, sub)
        ky2 = [
            kappa_squared(count * (row_id + at) + k, height) for k in range(count // 2 + 1)
        ]
        for c in range(columns):
            kx2 = kappa_squared(blocks * col + me * columns + c, width)
            here = slice(c * lane, (c + 1) * lane)
            for k in range(count // 2 + 1):
                for depth in range(depths):
                    real, imag = propagator((squared_ref[depth] - ky2[k]) - kx2, limit)
                    u_refs[depth][k, pl.ds(at, sub), here] = real
                    u_refs[depth][k, pl.ds(lane + at, sub), here] = imag
        return carry

    lax.fori_loop(0, lane // sub, wave_body, 0)


def waves(me, squared, after, lane, width, height, columns, limit):
    shape = (height // lane // 2 + 1, 2 * lane, columns * lane)
    return pl.pallas_call(
        functools.partial(
            wave_kernel, lane=lane, width=width, height=height, columns=columns, limit=limit
        ),
        in_specs=[SMEM, SMEM, ANY],
        out_specs=[FULL] * squared.shape[0],
        out_shape=[jax.ShapeDtypeStruct(shape, F32)] * squared.shape[0],
        compiler_params=params(),
        cost_estimate=cost(height * columns * lane * 8000, height * columns * lane * 16),
        name="waves",
    )(me, squared, after)


def spectral_kernel(*refs, lane, width, rows, devices, chunks):
    me_ref, u_ref, forward_ref, inverse_ref = refs[:4]
    ins = refs[4 : 4 + chunks * devices]
    outs = refs[4 + chunks * devices : 4 + 2 * chunks * devices]
    (
        in_ref, out_ref, edge_ref, x_ref, z_ref, w_ref, in_sem, out_sem, edge_sem,
    ) = refs[4 + 2 * chunks * devices :]
    me = me_ref[0]
    height = devices * rows
    part_rows = rows // chunks
    count = height // lane
    blocks = width // lane
    columns = blocks // devices
    sub = 16
    pair = 2 * lane

    def place_of(slot, h):
        start = lax.bitwise_xor(me, slot) * rows + h * part_rows
        return pl.multiple_of(start, 16)

    def copies(c):
        made = []
        for h in range(chunks):
            for slot in range(devices):
                made.append(
                    pltpu.make_async_copy(
                        ins[h * devices + slot].at[:, pl.ds(c * pair, pair)],
                        in_ref.at[c, pl.ds(place_of(slot, h), part_rows), :],
                        in_sem.at[c, h, slot],
                    )
                )
        return made

    arriving = [copies(c) for c in range(columns)]
    for group in arriving:
        for copy in group:
            copy.start()

    for c in range(columns):
        for copy in arriving[c]:
            copy.wait()
        here = slice(c * lane, (c + 1) * lane)

        def load_body(i, carry, c=c, here=here):
            at = pl.multiple_of(i * sub, sub)
            real, imag = [], []
            for b in range(count):
                row = pl.multiple_of(at + b * lane, sub)
                real.append(in_ref[c, pl.ds(row, sub), 0:lane].astype(F32))
                imag.append(in_ref[c, pl.ds(row, sub), lane:pair].astype(F32))
            real, imag = small_dft(real, imag, -1)
            for k in range(count):
                x_ref[k, pl.ds(at, sub), here] = real[k].astype(BF16)
                x_ref[k, pl.ds(lane + at, sub), here] = imag[k].astype(BF16)
            return carry

        lax.fori_loop(0, lane // sub, load_body, 0)

    for k in range(count):
        same = k if 2 * k <= count else count - k
        y = dot(forward_ref[k], x_ref[k])
        yr, yi = y[:lane], y[lane:]
        ur, ui = u_ref[same, 0:lane, :], u_ref[same, lane:pair, :]
        z_ref[k, 0:lane, :] = (yr * ur - yi * ui).astype(BF16)
        z_ref[k, lane:pair, :] = (yr * ui + yi * ur).astype(BF16)
    for k in range(count):
        w_ref[k] = dot(inverse_ref[k], z_ref[k])

    leaving = []
    edge = lax.broadcasted_iota(jnp.int32, (EXTRA, pair), 0)
    for c in range(columns):
        here = slice(c * lane, (c + 1) * lane)

        def store_body(i, carry, c=c, here=here):
            at = pl.multiple_of(i * sub, sub)
            real = [w_ref[k, pl.ds(at, sub), here] for k in range(count)]
            imag = [w_ref[k, pl.ds(lane + at, sub), here] for k in range(count)]
            real, imag = small_dft(real, imag, 1)
            for b in range(count):
                row = pl.multiple_of(at + b * lane, sub)
                out_ref[c, pl.ds(row, sub), 0:lane] = real[b].astype(BF16)
                out_ref[c, pl.ds(row, sub), lane:pair] = imag[b].astype(BF16)
            return carry

        lax.fori_loop(0, lane // sub, store_body, 0)

        def place(tile, row, source):
            return jnp.where(edge == row, jnp.broadcast_to(source.astype(F32), edge.shape), tile)

        for slab in range(devices):
            tile = jnp.zeros(edge.shape, F32)
            start = slab * rows
            after = out_ref[c, start + part_rows : start + part_rows + EXTRA, :].astype(F32)
            tile = place(tile, 0, after[0:1])
            if slab + 1 < devices:
                after = out_ref[c, start + rows : start + rows + EXTRA, :].astype(F32)
                tile = place(tile, 8, after[0:1])
            if slab:
                before = out_ref[c, start - EXTRA : start, :].astype(F32)
                tile = place(tile, EXTRA - 1, before[EXTRA - 1 :])
            edge_ref[c, slab] = tile.astype(BF16)
        for h in range(chunks):
            for slot in range(devices):
                target = outs[h * devices + slot]
                owner = lax.bitwise_xor(me, slot)
                leaving.append(
                    pltpu.make_async_copy(
                        out_ref.at[c, pl.ds(place_of(slot, h), part_rows), :],
                        target.at[pl.ds(0, part_rows), pl.ds(c * pair, pair)],
                        out_sem.at[c, h, slot],
                    )
                )
                leaving[-1].start()
                if h == 0:
                    leaving.append(
                        pltpu.make_async_copy(
                            edge_ref.at[c, owner],
                            target.at[pl.ds(part_rows, EXTRA), pl.ds(c * pair, pair)],
                            edge_sem.at[c, slot],
                        )
                    )
                    leaving[-1].start()
    for copy in leaving:
        copy.wait()


def spectral(me, waves, pieces, tables, lane, width):
    chunks, devices = len(pieces), len(pieces[0])
    part_rows, wide = pieces[0][0].shape
    rows = part_rows * chunks
    columns = wide // (2 * lane)
    height = devices * rows
    count = height // lane
    shapes = []
    for h in range(chunks):
        extra = EXTRA if h == 0 else 0
        shapes += [jax.ShapeDtypeStruct((part_rows + extra, wide), BF16)] * devices
    sent = pl.pallas_call(
        functools.partial(
            spectral_kernel, lane=lane, width=width, rows=rows, devices=devices, chunks=chunks
        ),
        in_specs=[SMEM, FULL, FULL, FULL] + [FULL] * (chunks * devices),
        out_specs=[FULL] * (chunks * devices),
        out_shape=shapes,
        scratch_shapes=[
            pltpu.VMEM((columns, height, 2 * lane), BF16),
            pltpu.VMEM((columns, height, 2 * lane), BF16),
            pltpu.VMEM((columns, devices, EXTRA, 2 * lane), BF16),
            pltpu.VMEM((count, 2 * lane, columns * lane), BF16),
            pltpu.VMEM((count, 2 * lane, columns * lane), BF16),
            pltpu.VMEM((count, 2 * lane, columns * lane), F32),
            pltpu.SemaphoreType.DMA((columns, chunks, devices)),
            pltpu.SemaphoreType.DMA((columns, chunks, devices)),
            pltpu.SemaphoreType.DMA((columns, devices)),
        ],
        compiler_params=params(),
        cost_estimate=cost(height * columns * lane * 8000, height * columns * lane * 16),
        name="spectral",
    )(me, waves, *tables, *[piece for part in pieces for piece in part])
    return [sent[h * devices : (h + 1) * devices] for h in range(chunks)]


def space_kernel(*refs, lane, devices, chunk, first, last):
    me_ref, factor_ref, coef_hbm, block_hbm, twist_ref, inverse_ref, forward_ref = refs[:7]
    ins = refs[7 : 7 + devices]
    at = 7 + devices
    if not first:
        carried_ref = refs[at]
        at += 1
    if last and not first:
        at += 1
    outs = refs[at : at + (1 if last else devices)]
    at += len(outs)
    kept_ref, sent_ref = refs[at : at + 2]
    at += 2
    if first:
        carry_ref = refs[at]
        at += 1
    (
        coef_ref, block_ref, y_ref, s_ref, left_ref, p_ref, fixed_sem, out_sem,
    ) = refs[at:]
    me = me_ref[0]
    padded, wide = ins[0].shape
    per_device = wide // (2 * lane)
    rows, width = coef_ref.shape
    blocks = width // lane
    pair = 2 * lane
    coef_copy = pltpu.make_async_copy(
        coef_hbm.at[pl.ds(chunk * rows, rows), :], coef_ref, fixed_sem.at[0]
    )
    block_copy = pltpu.make_async_copy(block_hbm, block_ref, fixed_sem.at[1])
    coef_copy.start()
    block_copy.start()

    for slot in range(devices):
        left = jnp.concatenate(
            [ins[slot][:, place * pair : (place + 1) * pair] for place in range(per_device)],
            axis=0,
        )
        owner = lax.bitwise_xor(me, slot)
        y_ref[pl.ds(owner * per_device, per_device)] = dot(left, inverse_ref[...]).reshape(
            per_device, padded, pair
        )

    def back(start, target):
        real, imag = [], []
        for k in range(blocks):
            re = y_ref[k, pl.ds(start, 8), 0:lane]
            im = y_ref[k, pl.ds(start, 8), lane:pair]
            if k:
                c, s = twist_ref[0, k : k + 1, :], twist_ref[1, k : k + 1, :]
                re, im = re * c + im * s, im * c - re * s
            real.append(re)
            imag.append(im)
        real, imag = small_dft(real, imag, 1)
        for b in range(blocks):
            here = slice(b * lane, (b + 1) * lane)
            s_ref[0, pl.ds(target, 8), here] = real[b]
            s_ref[1, pl.ds(target, 8), here] = imag[b]

    def back_body(i, carry):
        start = pl.multiple_of(i * 8, 8)
        back(start, pl.multiple_of(start + 8, 8))
        return carry

    if first:
        lax.fori_loop(0, rows // 8 + 1, back_body, 0)
        back(rows + 8, 0)
        carry_ref[:, 0:8, :] = s_ref[:, rows : rows + 8, :]
        carry_ref[:, 8:16, :] = s_ref[:, 0:8, :]
    else:
        lax.fori_loop(0, rows // 8, back_body, 0)
        s_ref[:, 0:8, :] = carried_ref[:, 0:8, :]
        s_ref[:, rows + 8 : rows + 16, :] = carried_ref[:, 8:16, :]

    coef_copy.wait()
    gr, gi = factor_ref[0], factor_ref[1]
    sub = 16

    def correct(i, carry):
        at = pl.multiple_of(i * sub, sub)
        for b in range(blocks):
            here = slice(b * lane, (b + 1) * lane)
            weight = coef_ref[pl.ds(at, sub), here].astype(F32)
            centre, curve = [], []
            for part in range(2):
                near = s_ref[part, pl.ds(at, sub + 16), here]
                mid, up, down = near[8 : 8 + sub], near[9 : 9 + sub], near[7 : 7 + sub]
                centre.append(mid)
                curve.append(up - 2.0 * mid + down)
            re = centre[0] + weight * (gr * curve[0] - gi * curve[1])
            im = centre[1] + weight * (gr * curve[1] + gi * curve[0])
            p_ref[0, pl.ds(at, sub), here] = re
            p_ref[1, pl.ds(at, sub), here] = im
            left_ref[b, pl.ds(at, sub), 0:lane] = re.astype(BF16)
            left_ref[b, pl.ds(at, sub), lane:pair] = im.astype(BF16)
        return carry

    lax.fori_loop(0, rows // sub, correct, 0)
    block_copy.wait()
    leaving = []
    half, _, share = kept_ref.shape
    stride = share // lane
    if stride:
        order = [
            (2 * z + parity) * stride + offset
            for z in range(half) for offset in range(stride) for parity in range(2)
        ]
    else:
        order = list(range(blocks))
    even = None
    for b in order:
        here = slice(b * lane, (b + 1) * lane)
        br, bi = block_ref[0, b], block_ref[1, b]
        square = jnp.concatenate(
            [jnp.concatenate([br, bi], axis=1), jnp.concatenate([-bi, br], axis=1)], axis=0
        )
        change = dot(left_ref[b], square)
        re = p_ref[0, :, here] + change[:, 0:lane]
        im = p_ref[1, :, here] + change[:, lane:pair]
        if not stride:
            per_tile = lane // share
            for piece in range(per_tile):
                owner = b * per_tile + piece
                value = re[:, piece * share : (piece + 1) * share].astype(BF16)
                place = lax.bitwise_xor(jnp.int32(owner // 2), me_ref[2])

                @pl.when(me_ref[1] == owner % 2)
                def _(place=place, value=value):
                    kept_ref[place] = value

                @pl.when(me_ref[1] != owner % 2)
                def _(place=place, value=value):
                    sent_ref[place] = value
        elif (b // stride) % 2 == 0:
            even = re
        else:
            place = lax.bitwise_xor(jnp.int32(b // stride // 2), me_ref[2])
            cols = slice((b % stride) * lane, (b % stride + 1) * lane)
            kept_ref[place, :, cols] = jnp.where(me_ref[1] == 0, even, re).astype(BF16)
            sent_ref[place, :, cols] = jnp.where(me_ref[1] == 0, re, even).astype(BF16)
        p_ref[0, :, here] = re
        p_ref[1, :, here] = im
        if last:
            leaving.append(
                pltpu.make_async_copy(
                    p_ref.at[:, :, pl.ds(b * lane, lane)],
                    outs[0].at[:, pl.ds(chunk * rows, rows), pl.ds(b * lane, lane)],
                    out_sem.at[b],
                )
            )
            leaving[-1].start()
    if not last:

        def load(part, at, b):
            return p_ref[part, at, b * lane : (b + 1) * lane]

        forward_lanes(load, rows, blocks, lane, twist_ref, left_ref)
        for slot in range(devices):
            parts = slot_products(left_ref, forward_ref, me, slot, per_device)
            for place, part in enumerate(parts):
                outs[slot][:, place * pair : (place + 1) * pair] = part
    for copy in leaving:
        copy.wait()


def space(me, pieces, coefficient, factor, inverse_blocks, tables, lane, chunk, carried, field,
          last):
    devices = len(pieces)
    padded, wide = pieces[0].shape
    first = chunk == 0
    rows = padded - EXTRA if first else padded
    all_rows, width = coefficient.shape
    blocks = width // lane
    if last:
        shapes = [jax.ShapeDtypeStruct((2, all_rows, width), F32)]
    else:
        shapes = [jax.ShapeDtypeStruct((rows, wide), BF16)] * devices
    specs = [ANY if last else FULL] * len(shapes)
    groups = lax.axis_size("freq")
    half = jax.ShapeDtypeStruct((groups // 2, rows, width // groups), BF16)
    shapes = shapes + [half, half]
    specs = specs + [FULL, FULL]
    if first:
        shapes = shapes + [jax.ShapeDtypeStruct((2, 16, width), F32)]
        specs = specs + [FULL]
    operands = [me, factor, coefficient, inverse_blocks, tables[2], tables[1], tables[0], *pieces]
    in_specs = [SMEM, SMEM, ANY, ANY, FULL, FULL, FULL] + [FULL] * devices
    aliases = {}
    if not first:
        operands.append(carried)
        in_specs.append(FULL)
        if last:
            aliases = {len(operands): 0}
            operands.append(field)
            in_specs.append(ANY)
    got = pl.pallas_call(
        functools.partial(
            space_kernel, lane=lane, devices=devices, chunk=chunk, first=first, last=last
        ),
        in_specs=in_specs,
        out_specs=specs,
        out_shape=shapes,
        scratch_shapes=[
            pltpu.VMEM((rows, width), BF16),
            pltpu.VMEM(inverse_blocks.shape, BF16),
            pltpu.VMEM((blocks, padded, 2 * lane), F32),
            pltpu.VMEM((2, rows + 16, width), F32),
            pltpu.VMEM((blocks, rows, 2 * lane), BF16),
            pltpu.VMEM((2, rows, width), F32),
            pltpu.SemaphoreType.DMA((2,)),
            pltpu.SemaphoreType.DMA((blocks,)),
        ],
        input_output_aliases=aliases,
        compiler_params=params(),
        cost_estimate=cost(rows * width * 8000, rows * width * 12),
        name="space_last" if last else "space",
    )(*operands)
    got = list(got)
    carry = got.pop() if first else None
    sent, kept = got.pop(), got.pop()
    image = (kept, sent)
    return (got[0] if last else got), image, carry


def swap(value, axis, distance):
    count = lax.axis_size(axis)
    return lax.ppermute(value, axis, [(i, i ^ distance) for i in range(count)])


def exchange(pieces):
    return [pieces[0]] + [swap(piece, "rows", k) for k, piece in enumerate(pieces) if k]


def add_all(value, axis, distances):
    return value + sum(swap(value, axis, distance) for distance in distances)


def collect(image):
    kept, sent = image
    joined = (kept.astype(F32) + swap(sent, "freq", 1).astype(F32)).astype(BF16)
    parts = [joined[0]]
    for j in range(1, joined.shape[0]):
        parts.append(swap(joined[j], "freq", 2 * j))
    return sum(part.astype(F32) for part in parts)


def total(value):
    groups, rows = lax.axis_size("freq"), lax.axis_size("rows")
    value = add_all(value, "freq", [1])
    value = add_all(value, "freq", range(2, groups, 2))
    return add_all(value, "rows", range(1, rows))


def shards(wavefield, block_inverse, coefficient, correction_factor, frequencies, slowness):
    freq_local, rows_local, width = wavefield.shape[1:]
    devices = lax.axis_size("rows")
    groups = lax.axis_size("freq")
    height = rows_local * devices
    lane = block_inverse.shape[-1]
    chunks = 2
    limit = (4.5 * 1.0) ** 2 * 1.0001
    x_tables = lane_tables(width, lane)
    y_tables = row_tables(height, lane)
    place = lax.axis_index("freq")
    me = jnp.stack([lax.axis_index("rows"), place % 2, place // 2]).astype(jnp.int32)
    partials = [[None] * chunks for _ in range(DEPTHS)]
    columns = width // lane // devices
    fields = []
    for f in range(freq_local):
        factor = correction_factor[:, f]
        made = [
            forward_x(me, wavefield[:, f], x_tables, lane, devices, h, chunks)
            for h in range(chunks)
        ]
        squared = (frequencies[f] * slowness) ** 2
        table = waves(me, squared, made[-1][0], lane, width, height, columns, limit)
        pieces = [exchange(part) for part in made]
        for depth_step in range(DEPTHS):
            last = depth_step == DEPTHS - 1
            sent = spectral(me, table[depth_step], pieces, y_tables, lane, width)
            arrived = [exchange(part) for part in sent]
            pieces, carry, field = [], None, None
            for h in range(chunks):
                made, image, carried = space(
                    me, arrived[h], coefficient, factor, block_inverse[:, f], x_tables, lane, h,
                    carry, field, last,
                )
                carry = carry if carried is None else carried
                if last:
                    field = made
                else:
                    pieces.append(exchange(made))
                before = partials[depth_step][h]
                if before is not None:
                    image = [
                        (a.astype(F32) + b.astype(F32)).astype(BF16)
                        for a, b in zip(before, image)
                    ]
                partials[depth_step][h] = image
        fields.append(field)
    shares = jnp.stack(
        [jnp.concatenate([collect(image) for image in images]) for images in partials]
    )
    energy = total(jnp.sum(shares * shares, axis=(1, 2)))
    scale = 1.0 / jnp.sqrt(energy / (height * width) + epsilon)
    return shares * scale[:, None, None], jnp.stack(fields, axis=1)


def solution(mesh):
    placed = (
        P(None, "freq", "rows", None),
        P(None, "freq", None, None, None),
        P("rows", None),
        P(None, "freq"),
        P("freq"),
        P(),
    )
    return jax.shard_map(
        shards,
        mesh=mesh,
        in_specs=placed,
        out_specs=(P(None, "rows", "freq"), P(None, "freq", "rows", None)),
        check_vma=False,
    )
```

```python
import functools
import math

import jax
import jax.numpy as jnp
import numpy as np
from jax import lax
from jax.experimental import pallas as pl
from jax.experimental.pallas import tpu as pltpu
from jax.sharding import PartitionSpec as P


DEPTHS = 2
epsilon = 1e-06
F32 = jnp.float32
BF16 = jnp.bfloat16
VMEM_LIMIT = 36 * 1024 * 1024
EXTRA = 16


def small_dft(real, imag, sign):
    count = len(real)
    if count == 1:
        return list(real), list(imag)
    even_r, even_i = small_dft(real[0::2], imag[0::2], sign)
    odd_r, odd_i = small_dft(real[1::2], imag[1::2], sign)
    half = count // 2
    out_r, out_i = [None] * count, [None] * count
    for k in range(half):
        br, bi = odd_r[k], odd_i[k]
        if k == 0:
            tr, ti = br, bi
        elif 4 * k == count:
            tr, ti = (-bi, br) if sign > 0 else (bi, -br)
            if sign > 0:
                out_r[k], out_i[k] = even_r[k] - bi, even_i[k] + br
                out_r[k + half], out_i[k + half] = even_r[k] + bi, even_i[k] - br
            else:
                out_r[k], out_i[k] = even_r[k] + bi, even_i[k] - br
                out_r[k + half], out_i[k + half] = even_r[k] - bi, even_i[k] + br
            continue
        else:
            angle = sign * 2.0 * math.pi * k / count
            c, s = math.cos(angle), math.sin(angle)
            if abs(abs(c) - abs(s)) < 1e-12:
                h = abs(c)
                cs, ss = math.copysign(1.0, c), math.copysign(1.0, s)
                re = (br if cs > 0 else -br) + (-bi if ss > 0 else bi)
                im = (bi if cs > 0 else -bi) + (br if ss > 0 else -br)
                tr, ti = re * h, im * h
            else:
                tr, ti = br * c - bi * s, br * s + bi * c
        out_r[k], out_i[k] = even_r[k] + tr, even_i[k] + ti
        out_r[k + half], out_i[k + half] = even_r[k] - tr, even_i[k] - ti
    return out_r, out_i


def lane_tables(width, lane):
    blocks = width // lane
    a = np.arange(lane)
    forward = np.exp(-2j * np.pi * np.outer(a, a) / lane)
    inverse = np.exp(2j * np.pi * np.outer(a, a) / lane) / width

    def embed(m):
        return np.block([[m.real, m.imag], [-m.imag, m.real]])

    twist = np.exp(-2j * np.pi * np.outer(np.arange(blocks), a) / width)
    return (
        jnp.asarray(embed(forward), BF16),
        jnp.asarray(embed(inverse), BF16),
        jnp.asarray(np.stack([twist.real, twist.imag]), F32),
    )


def row_tables(height, lane):
    count = height // lane
    a = np.arange(lane)
    forward, inverse = [], []
    for k in range(count):
        j = a if 2 * k <= count else lane - 1 - a
        ky = count * j + k
        table = np.exp(-2j * np.pi * np.outer(ky, a) / height)
        forward.append(np.block([[table.real, -table.imag], [table.imag, table.real]]))
        back = np.conj(table.T) / height
        inverse.append(np.block([[back.real, -back.imag], [back.imag, back.real]]))
    return jnp.asarray(np.stack(forward), BF16), jnp.asarray(np.stack(inverse), BF16)


def dot(left, right):
    return jnp.dot(left, right, preferred_element_type=F32)


ANY = pl.BlockSpec(memory_space=pltpu.HBM)
SMEM = pl.BlockSpec(memory_space=pltpu.SMEM)
FULL = pl.BlockSpec(memory_space=pltpu.VMEM)


def cost(flops, moved):
    return pl.CostEstimate(flops=flops, bytes_accessed=moved, transcendentals=0)


def params(limit=VMEM_LIMIT):
    return pltpu.CompilerParams(vmem_limit_bytes=limit)


def forward_lanes(load, rows, blocks, lane, twist_ref, left_ref, base=0):
    sub = 16

    def body(i, carry):
        at = pl.ds(pl.multiple_of(i * sub, sub), sub)
        to = pl.ds(pl.multiple_of(i * sub + base, sub), sub)
        real = [load(0, at, b) for b in range(blocks)]
        imag = [load(1, at, b) for b in range(blocks)]
        real, imag = small_dft(real, imag, -1)
        for k in range(blocks):
            if k:
                c, s = twist_ref[0, k : k + 1, :], twist_ref[1, k : k + 1, :]
                re, im = real[k] * c - imag[k] * s, real[k] * s + imag[k] * c
            else:
                re, im = real[k], imag[k]
            left_ref[k, to, 0:lane] = re.astype(BF16)
            left_ref[k, to, lane : 2 * lane] = im.astype(BF16)
        return carry

    lax.fori_loop(0, rows // sub, body, 0)


def slot_products(left_ref, table_ref, me, slot, per_device):
    owner = lax.bitwise_xor(me, slot)
    left = left_ref[pl.ds(owner * per_device, per_device)]
    count, rows, wide = left.shape
    part = dot(left.reshape(count * rows, wide), table_ref[...]).astype(BF16)
    return [part[place * rows : (place + 1) * rows] for place in range(per_device)]


def store_slots(outs, left_ref, table_ref, me, per_device, lane):
    pair = 2 * lane
    span = outs[0].shape[1] // pair
    devices = len(outs) * span // per_device
    for slot in range(devices):
        made = slot_products(left_ref, table_ref, me, slot, per_device)
        for place, part in enumerate(made):
            target = outs[place // span * devices + slot]
            target[:, place % span * pair : (place % span + 1) * pair] = part


def first_kernel(*refs, lane, per_device, chunk, parts):
    me_ref, field_hbm, twist_hbm, table_hbm, _ = refs[:5]
    outs = refs[5:-5]
    field_ref, left_ref, twist_ref, table_ref, sem = refs[-5:]
    rows, width = field_ref.shape[1], field_ref.shape[2]
    tile = rows // parts
    arriving = [
        pltpu.make_async_copy(
            field_hbm.at[:, pl.ds(chunk * rows + t * tile, tile), :],
            field_ref.at[:, pl.ds(t * tile, tile), :],
            sem.at[t],
        )
        for t in range(parts)
    ]
    twist_in = pltpu.make_async_copy(twist_hbm, twist_ref, sem.at[parts])
    table_in = pltpu.make_async_copy(table_hbm, table_ref, sem.at[parts + 1])
    twist_in.start()
    for copy in arriving:
        copy.start()
    table_in.start()
    twist_in.wait()
    for t in range(parts):
        arriving[t].wait()

        def load(part, at, b, t=t):
            return field_ref[part, pl.ds(at.start + t * tile, at.size), b * lane : (b + 1) * lane]

        forward_lanes(load, tile, width // lane, lane, twist_ref, left_ref, t * tile)
    table_in.wait()
    store_slots(outs, left_ref, table_ref, me_ref[0], per_device, lane)


def forward_x(me, field, tables, lane, devices, chunk, chunks, pieces, after):
    _, rows, width = field.shape
    blocks = width // lane
    per_device = blocks // devices
    rows = rows // chunks
    parts = max(rows // 32, 1)
    shape = jax.ShapeDtypeStruct((rows, per_device * 2 * lane // pieces), BF16)
    made = pl.pallas_call(
        functools.partial(
            first_kernel, lane=lane, per_device=per_device, chunk=chunk, parts=parts
        ),
        in_specs=[SMEM, ANY, ANY, ANY, pl.BlockSpec(memory_space=pl.ANY)],
        out_specs=[FULL] * (devices * pieces),
        out_shape=[shape] * (devices * pieces),
        scratch_shapes=[
            pltpu.VMEM((2, rows, width), F32),
            pltpu.VMEM((blocks, rows, 2 * lane), BF16),
            pltpu.VMEM(tables[2].shape, F32),
            pltpu.VMEM(tables[0].shape, BF16),
            pltpu.SemaphoreType.DMA((parts + 2,)),
        ],
        compiler_params=params(60 * 1024 * 1024),
        cost_estimate=cost(rows * width * 4000, rows * width * 12),
        name="forward_x",
    )(me, field, tables[2], tables[0], after)
    return [made[p * devices : (p + 1) * devices] for p in range(pieces)]


def poly(coefficients, t):
    acc = jnp.full_like(t, coefficients[-1])
    for c in coefficients[-2::-1]:
        acc = acc * t + c
    return acc


@functools.lru_cache(maxsize=None)
def wave_series(limit):
    from numpy.polynomial import chebyshev

    nodes = np.cos(np.pi * (np.arange(64) + 0.5) / 64)
    root = np.sqrt((nodes + 1.0) * 0.5 * limit)
    out = []
    for values in (np.cos(root), np.sinc(root / np.pi)):
        fitted = chebyshev.chebfit(nodes, values, 7)
        out.append(tuple(float(c) for c in chebyshev.cheb2poly(fitted)))
    return tuple(out)


def propagator(q, limit):
    root = jnp.sqrt(jnp.abs(q))
    t = q * (2.0 / limit) - 1.0
    cosine, sinc = wave_series(limit)
    upward = q >= 0.0
    t = jnp.where(upward, t, 0.0)
    real = jnp.where(upward, poly(cosine, t), jnp.exp(-root))
    imag = jnp.where(upward, root * poly(sinc, t), 0.0)
    return real, imag


def wave_kernel(me_ref, squared_ref, after_ref, *u_refs, lane, width, height, columns, limit):
    me = me_ref[0]
    depths = squared_ref.shape[0]
    parts = len(u_refs) // depths
    span = columns // parts
    count = height // lane
    blocks = width // lane
    sub = 8
    col = lax.broadcasted_iota(jnp.int32, (sub, lane), 1)
    row_id = lax.broadcasted_iota(jnp.int32, (sub, lane), 0)

    def kappa_squared(index, length):
        signed = jnp.where(2 * index < length, index, index - length)
        kappa = signed.astype(F32) * (2.0 * math.pi / length)
        return kappa * kappa

    def wave_body(i, carry):
        at = pl.multiple_of(i * sub, sub)
        ky2 = [
            kappa_squared(count * (row_id + at) + k, height) for k in range(count // 2 + 1)
        ]
        for c in range(columns):
            kx2 = kappa_squared(blocks * col + me * columns + c, width)
            here = slice(c % span * lane, (c % span + 1) * lane)
            for k in range(count // 2 + 1):
                for depth in range(depths):
                    real, imag = propagator((squared_ref[depth] - ky2[k]) - kx2, limit)
                    u_refs[depth * parts + c // span][k, pl.ds(at, sub), here] = real
                    u_refs[depth * parts + c // span][k, pl.ds(lane + at, sub), here] = imag
        return carry

    lax.fori_loop(0, lane // sub, wave_body, 0)


def waves(me, squared, after, lane, width, height, columns, limit, parts):
    shape = (height // lane // 2 + 1, 2 * lane, columns * lane // parts)
    many = squared.shape[0] * parts
    return pl.pallas_call(
        functools.partial(
            wave_kernel, lane=lane, width=width, height=height, columns=columns, limit=limit
        ),
        in_specs=[SMEM, SMEM, pl.BlockSpec(memory_space=pl.ANY)],
        out_specs=[FULL] * many,
        out_shape=[jax.ShapeDtypeStruct(shape, F32)] * many,
        compiler_params=params(),
        cost_estimate=cost(height * columns * lane * 8000, height * columns * lane * 16),
        name="waves",
    )(me, squared, after)


def xor_permute(values, me):
    values = list(values)
    bit = 1
    while bit < len(values):
        taken = lax.bitwise_and(me, jnp.int32(bit)) != 0
        values = [jnp.where(taken, values[k ^ bit], values[k]) for k in range(len(values))]
        bit *= 2
    return values


def spectral_kernel(*refs, lane, width, devices, chunks, part, parts, tiled):
    me_ref, u_ref, forward_ref, inverse_ref = refs[:4]
    refs = refs[4:]
    total_in = chunks * devices
    ins = [refs[h * devices : (h + 1) * devices] for h in range(chunks)]
    refs = refs[total_in:]
    joins = part == parts - 1 and parts > 1
    if joins:
        priors, refs = refs[:devices], refs[devices:]
    outs = [refs[h * devices : (h + 1) * devices] for h in range(chunks)]
    refs = refs[total_in:]
    x_ref, z_ref, w_ref = refs[:3]
    me = me_ref[0]
    part_rows = ins[0][0].shape[0]
    rows = part_rows * chunks
    height = devices * rows
    count = height // lane
    pair = 2 * lane
    columns = outs[0][0].shape[1] // pair
    sub = 16
    span = columns * pair
    in_base = [part * span] + [0] * (chunks - 1)
    out_base = [0] + [part * span if joins else 0] * (chunks - 1)
    if not tiled:
        in_ref, out_ref, in_sem, out_sem = refs[3:]

        def place_of(slot, h):
            start = lax.bitwise_xor(me, slot) * rows + h * part_rows
            return pl.multiple_of(start, 16)

        def moves(h, slot, inward):
            near = (in_ref if inward else out_ref).at[pl.ds(place_of(slot, h), part_rows), :]
            if inward:
                far = ins[h][slot].at[:, pl.ds(in_base[h], span)]
                return pltpu.make_async_copy(far, near, in_sem.at[h, slot])
            far = outs[h][slot].at[pl.ds(0, part_rows), pl.ds(out_base[h], span)]
            return pltpu.make_async_copy(near, far, out_sem.at[h, slot])

        arriving = [moves(h, k, True) for h in range(chunks) for k in range(devices)]
        for copy in arriving:
            copy.start()
        for copy in arriving:
            copy.wait()
    per_chunk = part_rows // lane

    def fetch(at, base):
        if not tiled:
            return [
                in_ref[pl.ds(pl.multiple_of(at + b * lane, sub), sub), base : base + pair]
                for b in range(count)
            ]
        found = [None] * count
        for h in range(chunks):
            lanes = slice(in_base[h] + base, in_base[h] + base + pair)
            for t in range(per_chunk):
                got = xor_permute(
                    [ref[pl.ds(pl.multiple_of(at + t * lane, sub), sub), lanes] for ref in ins[h]],
                    me,
                )
                for slab in range(devices):
                    found[(slab * chunks + h) * per_chunk + t] = got[slab]
        return found

    def leave(at, base, values):
        if not tiled:
            for b in range(count):
                row = pl.multiple_of(at + b * lane, sub)
                out_ref[pl.ds(row, sub), base : base + pair] = values[b]
            return
        for h in range(chunks):
            lanes = slice(out_base[h] + base, out_base[h] + base + pair)
            for t in range(per_chunk):
                got = xor_permute(
                    [values[(slab * chunks + h) * per_chunk + t] for slab in range(devices)], me
                )
                for slot in range(devices):
                    row = pl.multiple_of(at + t * lane, sub)
                    outs[h][slot][pl.ds(row, sub), lanes] = got[slot]

    for c in range(columns):
        here = slice(c * lane, (c + 1) * lane)

        def load_body(i, carry, c=c, here=here):
            at = pl.multiple_of(i * sub, sub)
            tiles = [tile.astype(F32) for tile in fetch(at, c * pair)]
            real, imag = small_dft(
                [tile[:, :lane] for tile in tiles], [tile[:, lane:] for tile in tiles], -1
            )
            for k in range(count):
                x_ref[k, pl.ds(at, sub), here] = real[k].astype(BF16)
                x_ref[k, pl.ds(lane + at, sub), here] = imag[k].astype(BF16)
            return carry

        lax.fori_loop(0, lane // sub, load_body, 0)

    for k in range(count):
        same = k if 2 * k <= count else count - k
        y = dot(forward_ref[k], x_ref[k])
        yr, yi = y[:lane], y[lane:]
        ur, ui = u_ref[same, 0:lane, :], u_ref[same, lane:pair, :]
        z_ref[k, 0:lane, :] = (yr * ur - yi * ui).astype(BF16)
        z_ref[k, lane:pair, :] = (yr * ui + yi * ur).astype(BF16)
    for k in range(count):
        w_ref[k] = dot(inverse_ref[k], z_ref[k])

    for c in range(columns):
        here = slice(c * lane, (c + 1) * lane)

        def store_body(i, carry, c=c, here=here):
            at = pl.multiple_of(i * sub, sub)
            real = [w_ref[k, pl.ds(at, sub), here] for k in range(count)]
            imag = [w_ref[k, pl.ds(lane + at, sub), here] for k in range(count)]
            real, imag = small_dft(real, imag, 1)
            leave(
                at,
                c * pair,
                [
                    jnp.concatenate([re.astype(BF16), im.astype(BF16)], axis=1)
                    for re, im in zip(real, imag)
                ],
            )
            return carry

        lax.fori_loop(0, lane // sub, store_body, 0)
    if joins:
        for slot in range(devices):
            for h in range(1, chunks):
                outs[h][slot][:, 0 : part * span] = priors[slot][...]
    if not tiled:
        leaving = [moves(h, k, False) for h in range(chunks) for k in range(devices)]
        for copy in leaving:
            copy.start()
        for copy in leaving:
            copy.wait()

    edge = lax.broadcasted_iota(jnp.int32, (EXTRA, span), 0)
    tail = slice(out_base[-1], out_base[-1] + span)
    starts = [outs[0][k][0:EXTRA, :].astype(F32)[0:1] for k in range(devices)]
    ends = [
        outs[-1][k][part_rows - EXTRA : part_rows, tail].astype(F32)[EXTRA - 1 :]
        for k in range(devices)
    ]
    zero = [jnp.zeros((1, span), F32)]
    nexts = xor_permute(xor_permute(starts, me)[1:] + zero, me)
    lasts = xor_permute(zero + xor_permute(ends, me)[:-1], me)
    for k in range(devices):
        after = outs[1][k][0:EXTRA, out_base[1] : out_base[1] + span].astype(F32)[0:1]
        tile = jnp.zeros(edge.shape, F32)
        for row, value in ((0, after), (8, nexts[k]), (EXTRA - 1, lasts[k])):
            tile = jnp.where(edge == row, jnp.broadcast_to(value, edge.shape), tile)
        outs[0][k][part_rows : part_rows + EXTRA, :] = tile.astype(BF16)


def spectral(me, waves, pieces, priors, tables, lane, width, part, parts):
    chunks, devices = len(pieces), len(pieces[0])
    part_rows, wide = pieces[0][0].shape
    rows = part_rows * chunks
    span = wide // parts
    columns = span // (2 * lane)
    height = devices * rows
    count = height // lane
    tiled = part_rows % lane == 0
    joins = part == parts - 1 and parts > 1
    shapes = []
    for h in range(chunks):
        shape = (part_rows, wide if joins else span) if h else (part_rows + EXTRA, span)
        shapes += [jax.ShapeDtypeStruct(shape, BF16)] * devices
    operands = [piece for group in pieces for piece in group]
    if joins:
        operands += priors
    scratch = [
        pltpu.VMEM((count, 2 * lane, columns * lane), BF16),
        pltpu.VMEM((count, 2 * lane, columns * lane), BF16),
        pltpu.VMEM((count, 2 * lane, columns * lane), F32),
    ]
    if not tiled:
        scratch += [pltpu.VMEM((height, span), BF16)] * 2
        scratch += [pltpu.SemaphoreType.DMA((chunks, devices))] * 2
    sent = pl.pallas_call(
        functools.partial(
            spectral_kernel, lane=lane, width=width, devices=devices, chunks=chunks, part=part,
            parts=parts, tiled=tiled,
        ),
        in_specs=[SMEM, FULL, FULL, FULL] + [FULL] * len(operands),
        out_specs=[FULL] * (chunks * devices),
        out_shape=shapes,
        scratch_shapes=scratch,
        compiler_params=params(),
        cost_estimate=cost(height * columns * lane * 8000, height * columns * lane * 16),
        name="spectral",
    )(me, waves, *tables, *operands)
    return [sent[h * devices : (h + 1) * devices] for h in range(chunks)]


def space_kernel(*refs, lane, devices, groups_in, groups_out, chunk, first, last):
    me_ref, factor_ref, coef_hbm, block_hbm, twist_ref, inverse_ref, forward_ref = refs[:7]
    ins = refs[7 : 7 + groups_in * devices]
    at = 7 + groups_in * devices
    if not first:
        carried_ref = refs[at]
        at += 1
    if last and not first:
        at += 1
    outs = refs[at : at + (1 if last else groups_out * devices)]
    at += len(outs)
    kept_ref, sent_ref = refs[at : at + 2]
    at += 2
    if first:
        carry_ref = refs[at]
        at += 1
    (
        coef_ref, block_ref, y_ref, s_ref, left_ref, p_ref, fixed_sem, out_sem,
    ) = refs[at:]
    me = me_ref[0]
    padded, wide = ins[0].shape
    span = wide // (2 * lane)
    per_device = span * groups_in
    rows, width = coef_ref.shape
    blocks = width // lane
    pair = 2 * lane
    coef_copy = pltpu.make_async_copy(
        coef_hbm.at[pl.ds(chunk * rows, rows), :], coef_ref, fixed_sem.at[0]
    )
    block_copy = pltpu.make_async_copy(block_hbm, block_ref, fixed_sem.at[1])
    coef_copy.start()
    block_copy.start()

    for slot in range(devices):
        left = jnp.concatenate(
            [
                ins[place // span * devices + slot][
                    :, place % span * pair : (place % span + 1) * pair
                ]
                for place in range(per_device)
            ],
            axis=0,
        )
        owner = lax.bitwise_xor(me, slot)
        y_ref[pl.ds(owner * per_device, per_device)] = dot(left, inverse_ref[...]).reshape(
            per_device, padded, pair
        )

    def back(start, target):
        real, imag = [], []
        for k in range(blocks):
            re = y_ref[k, pl.ds(start, 8), 0:lane]
            im = y_ref[k, pl.ds(start, 8), lane:pair]
            if k:
                c, s = twist_ref[0, k : k + 1, :], twist_ref[1, k : k + 1, :]
                re, im = re * c + im * s, im * c - re * s
            real.append(re)
            imag.append(im)
        real, imag = small_dft(real, imag, 1)
        for b in range(blocks):
            here = slice(b * lane, (b + 1) * lane)
            s_ref[0, pl.ds(target, 8), here] = real[b]
            s_ref[1, pl.ds(target, 8), here] = imag[b]

    def back_body(i, carry):
        start = pl.multiple_of(i * 8, 8)
        back(start, pl.multiple_of(start + 8, 8))
        return carry

    if first:
        lax.fori_loop(0, rows // 8 + 1, back_body, 0)
        back(rows + 8, 0)
        carry_ref[:, 0:8, :] = s_ref[:, rows : rows + 8, :]
        carry_ref[:, 8:16, :] = s_ref[:, 0:8, :]
    else:
        lax.fori_loop(0, rows // 8, back_body, 0)
        s_ref[:, 0:8, :] = carried_ref[:, 0:8, :]
        s_ref[:, rows + 8 : rows + 16, :] = carried_ref[:, 8:16, :]

    coef_copy.wait()
    gr, gi = factor_ref[0], factor_ref[1]
    sub = 16

    def correct(i, carry):
        at = pl.multiple_of(i * sub, sub)
        for b in range(blocks):
            here = slice(b * lane, (b + 1) * lane)
            weight = coef_ref[pl.ds(at, sub), here].astype(F32)
            centre, curve = [], []
            for part in range(2):
                near = s_ref[part, pl.ds(at, sub + 16), here]
                mid, up, down = near[8 : 8 + sub], near[9 : 9 + sub], near[7 : 7 + sub]
                centre.append(mid)
                curve.append(up - 2.0 * mid + down)
            re = centre[0] + weight * (gr * curve[0] - gi * curve[1])
            im = centre[1] + weight * (gr * curve[1] + gi * curve[0])
            p_ref[0, pl.ds(at, sub), here] = re
            p_ref[1, pl.ds(at, sub), here] = im
            left_ref[b, pl.ds(at, sub), 0:lane] = re.astype(BF16)
            left_ref[b, pl.ds(at, sub), lane:pair] = im.astype(BF16)
        return carry

    lax.fori_loop(0, rows // sub, correct, 0)
    block_copy.wait()
    leaving = []
    half, _, share = kept_ref.shape
    stride = share // lane
    if stride:
        order = [
            (2 * z + parity) * stride + offset
            for z in range(half) for offset in range(stride) for parity in range(2)
        ]
    else:
        order = list(range(blocks))
    even = None
    for b in order:
        here = slice(b * lane, (b + 1) * lane)
        br, bi = block_ref[0, b], block_ref[1, b]
        square = jnp.concatenate(
            [jnp.concatenate([br, bi], axis=1), jnp.concatenate([-bi, br], axis=1)], axis=0
        )
        change = dot(left_ref[b], square)
        re = p_ref[0, :, here] + change[:, 0:lane]
        im = p_ref[1, :, here] + change[:, lane:pair]
        if not stride:
            per_tile = lane // share
            for piece in range(per_tile):
                owner = b * per_tile + piece
                value = re[:, piece * share : (piece + 1) * share].astype(BF16)
                place = lax.bitwise_xor(jnp.int32(owner // 2), me_ref[2])

                @pl.when(me_ref[1] == owner % 2)
                def _(place=place, value=value):
                    kept_ref[place] = value

                @pl.when(me_ref[1] != owner % 2)
                def _(place=place, value=value):
                    sent_ref[place] = value
        elif (b // stride) % 2 == 0:
            even = re
        else:
            place = lax.bitwise_xor(jnp.int32(b // stride // 2), me_ref[2])
            cols = slice((b % stride) * lane, (b % stride + 1) * lane)
            kept_ref[place, :, cols] = jnp.where(me_ref[1] == 0, even, re).astype(BF16)
            sent_ref[place, :, cols] = jnp.where(me_ref[1] == 0, re, even).astype(BF16)
        p_ref[0, :, here] = re
        p_ref[1, :, here] = im
        if last:
            leaving.append(
                pltpu.make_async_copy(
                    p_ref.at[:, :, pl.ds(b * lane, lane)],
                    outs[0].at[:, pl.ds(chunk * rows, rows), pl.ds(b * lane, lane)],
                    out_sem.at[b],
                )
            )
            leaving[-1].start()
    if not last:

        def load(part, at, b):
            return p_ref[part, at, b * lane : (b + 1) * lane]

        forward_lanes(load, rows, blocks, lane, twist_ref, left_ref)
        store_slots(outs, left_ref, forward_ref, me, per_device, lane)
    for copy in leaving:
        copy.wait()


def space(me, groups_in, coefficient, factor, inverse_blocks, tables, lane, chunk, carried,
          field, last, groups_out):
    devices = len(groups_in[0])
    pieces = [piece for group in groups_in for piece in group]
    padded, wide = pieces[0].shape
    wide = wide * len(groups_in)
    first = chunk == 0
    rows = padded - EXTRA if first else padded
    all_rows, width = coefficient.shape
    blocks = width // lane
    if last:
        shapes = [jax.ShapeDtypeStruct((2, all_rows, width), F32)]
    else:
        shape = jax.ShapeDtypeStruct((rows, wide // groups_out), BF16)
        shapes = [shape] * (devices * groups_out)
    specs = [ANY if last else FULL] * len(shapes)
    groups = lax.axis_size("freq")
    half = jax.ShapeDtypeStruct((groups // 2, rows, width // groups), BF16)
    shapes = shapes + [half, half]
    specs = specs + [FULL, FULL]
    if first:
        shapes = shapes + [jax.ShapeDtypeStruct((2, 16, width), F32)]
        specs = specs + [FULL]
    operands = [me, factor, coefficient, inverse_blocks, tables[2], tables[1], tables[0], *pieces]
    in_specs = [SMEM, SMEM, ANY, ANY, FULL, FULL, FULL] + [FULL] * len(pieces)
    aliases = {}
    if not first:
        operands.append(carried)
        in_specs.append(FULL)
        if last:
            aliases = {len(operands): 0}
            operands.append(field)
            in_specs.append(ANY)
    got = pl.pallas_call(
        functools.partial(
            space_kernel, lane=lane, devices=devices, groups_in=len(groups_in),
            groups_out=groups_out, chunk=chunk, first=first, last=last,
        ),
        in_specs=in_specs,
        out_specs=specs,
        out_shape=shapes,
        scratch_shapes=[
            pltpu.VMEM((rows, width), BF16),
            pltpu.VMEM(inverse_blocks.shape, BF16),
            pltpu.VMEM((blocks, padded, 2 * lane), F32),
            pltpu.VMEM((2, rows + 16, width), F32),
            pltpu.VMEM((blocks, rows, 2 * lane), BF16),
            pltpu.VMEM((2, rows, width), F32),
            pltpu.SemaphoreType.DMA((2,)),
            pltpu.SemaphoreType.DMA((blocks,)),
        ],
        input_output_aliases=aliases,
        compiler_params=params(),
        cost_estimate=cost(rows * width * 8000, rows * width * 12),
        name="space_last" if last else "space",
    )(*operands)
    got = list(got)
    carry = got.pop() if first else None
    sent, kept = got.pop(), got.pop()
    image = (kept, sent)
    if last:
        return got[0], image, carry
    return [got[p * devices : (p + 1) * devices] for p in range(groups_out)], image, carry


def swap(value, axis, distance):
    count = lax.axis_size(axis)
    return lax.ppermute(value, axis, [(i, i ^ distance) for i in range(count)])


def exchange(pieces):
    return [pieces[0]] + [swap(piece, "rows", k) for k, piece in enumerate(pieces) if k]


def add_all(value, axis, distances):
    return value + sum(swap(value, axis, distance) for distance in distances)


def collect(images):
    joined = []
    for kept, sent in images:
        other = swap(sent, "freq", 1)
        joined.append((kept.astype(F32) + other.astype(F32)).astype(BF16))
    parts = [jnp.concatenate([join[j] for join in joined]) for j in range(joined[0].shape[0])]
    for j in range(1, len(parts)):
        parts[j] = swap(parts[j], "freq", 2 * j)
    return sum(part.astype(F32) for part in parts)


def total(value):
    groups, rows = lax.axis_size("freq"), lax.axis_size("rows")
    value = add_all(value, "freq", [1])
    value = add_all(value, "freq", range(2, groups, 2))
    return add_all(value, "rows", range(1, rows))


def shards(wavefield, block_inverse, coefficient, correction_factor, frequencies, slowness):
    freq_local, rows_local, width = wavefield.shape[1:]
    devices = lax.axis_size("rows")
    height = rows_local * devices
    lane = block_inverse.shape[-1]
    chunks = 2
    limit = (4.5 * 1.0) ** 2 * 1.0001
    x_tables = lane_tables(width, lane)
    y_tables = row_tables(height, lane)
    place = lax.axis_index("freq")
    me = jnp.stack([lax.axis_index("rows"), place % 2, place // 2]).astype(jnp.int32)
    partials = [[None] * chunks for _ in range(DEPTHS)]
    columns = width // lane // devices
    parts = 2 if columns % 2 == 0 else 1
    fields = []
    for f in range(freq_local):
        factor = correction_factor[:, f]
        made, behind = [], me
        for h in range(chunks):
            made.append(
                forward_x(
                    me, wavefield[:, f], x_tables, lane, devices, h, chunks, parts if h else 1,
                    behind,
                )
            )
            behind = made[-1][0][0]
        squared = (frequencies[f] * slowness) ** 2
        table = waves(
            me, squared, made[-1][0][0], lane, width, height, columns, limit, parts
        )
        arrived = [[exchange(group) for group in groups] for groups in made]
        for depth_step in range(DEPTHS):
            last = depth_step == DEPTHS - 1
            leaving, priors = [[], []], None
            for p in range(parts):
                sent = spectral(
                    me, table[depth_step * parts + p], [arrived[0][0], arrived[1][p]],
                    priors, y_tables, lane, width, p, parts,
                )
                leaving[0].append(exchange(sent[0]))
                priors = sent[1]
            leaving[1].append(exchange(priors))
            arrived, carry, field = [], None, None
            for h in range(chunks):
                groups_out = parts if h else 1
                made, image, carried = space(
                    me, leaving[h], coefficient, factor, block_inverse[:, f], x_tables, lane,
                    h, carry, field, last, groups_out,
                )
                carry = carry if carried is None else carried
                if last:
                    field = made
                else:
                    arrived.append([exchange(group) for group in made])
                before = partials[depth_step][h]
                if before is not None:
                    image = [
                        (a.astype(F32) + b.astype(F32)).astype(BF16)
                        for a, b in zip(before, image)
                    ]
                partials[depth_step][h] = image
        fields.append(field)
    shares = []
    for d, images in enumerate(partials):
        if d < DEPTHS - 1:
            shares.append(collect(images))
        else:
            shares.append(jnp.concatenate([collect([image]) for image in images]))
    shares = jnp.stack(shares)
    energy = total(jnp.sum(shares * shares, axis=(1, 2)))
    scale = 1.0 / jnp.sqrt(energy / (height * width) + epsilon)
    return shares * scale[:, None, None], jnp.stack(fields, axis=1)


def solution(mesh):
    placed = (
        P(None, "freq", "rows", None),
        P(None, "freq", None, None, None),
        P("rows", None),
        P(None, "freq"),
        P("freq"),
        P(),
    )

    return jax.shard_map(
        shards,
        mesh=mesh,
        in_specs=placed,
        out_specs=(P(None, "rows", "freq"), P(None, "freq", "rows", None)),
        check_vma=False,
    )
```

```python
import functools
import math

import jax
import jax.numpy as jnp
import numpy as np
from jax import lax
from jax.experimental import pallas as pl
from jax.experimental.pallas import tpu as pltpu
from jax.sharding import PartitionSpec as P


DEPTHS = 2
epsilon = 1e-06
F32 = jnp.float32
BF16 = jnp.bfloat16
VMEM_LIMIT = 36 * 1024 * 1024
EXTRA = 16


def small_dft(real, imag, sign):
    count = len(real)
    if count == 1:
        return list(real), list(imag)
    even_r, even_i = small_dft(real[0::2], imag[0::2], sign)
    odd_r, odd_i = small_dft(real[1::2], imag[1::2], sign)
    half = count // 2
    out_r, out_i = [None] * count, [None] * count
    for k in range(half):
        br, bi = odd_r[k], odd_i[k]
        if k == 0:
            tr, ti = br, bi
        elif 4 * k == count:
            tr, ti = (-bi, br) if sign > 0 else (bi, -br)
            if sign > 0:
                out_r[k], out_i[k] = even_r[k] - bi, even_i[k] + br
                out_r[k + half], out_i[k + half] = even_r[k] + bi, even_i[k] - br
            else:
                out_r[k], out_i[k] = even_r[k] + bi, even_i[k] - br
                out_r[k + half], out_i[k + half] = even_r[k] - bi, even_i[k] + br
            continue
        else:
            angle = sign * 2.0 * math.pi * k / count
            c, s = math.cos(angle), math.sin(angle)
            if abs(abs(c) - abs(s)) < 1e-12:
                h = abs(c)
                cs, ss = math.copysign(1.0, c), math.copysign(1.0, s)
                re = (br if cs > 0 else -br) + (-bi if ss > 0 else bi)
                im = (bi if cs > 0 else -bi) + (br if ss > 0 else -br)
                tr, ti = re * h, im * h
            else:
                tr, ti = br * c - bi * s, br * s + bi * c
        out_r[k], out_i[k] = even_r[k] + tr, even_i[k] + ti
        out_r[k + half], out_i[k + half] = even_r[k] - tr, even_i[k] - ti
    return out_r, out_i


def lane_tables(width, lane):
    blocks = width // lane
    a = np.arange(lane)
    forward = np.exp(-2j * np.pi * np.outer(a, a) / lane)
    inverse = np.exp(2j * np.pi * np.outer(a, a) / lane) / width

    def embed(m):
        return np.block([[m.real, m.imag], [-m.imag, m.real]])

    twist = np.exp(-2j * np.pi * np.outer(np.arange(blocks), a) / width)
    return (
        jnp.asarray(embed(forward), BF16),
        jnp.asarray(embed(inverse), BF16),
        jnp.asarray(np.stack([twist.real, twist.imag]), F32),
    )


def row_tables(height, lane):
    count = height // lane
    a = np.arange(lane)
    forward, inverse = [], []
    for k in range(count // 2 + 1):
        ky = count * a + k
        table = np.exp(-2j * np.pi * np.outer(ky, a) / height)
        forward.append(np.block([[table.real, -table.imag], [table.imag, table.real]]))
        back = np.conj(table.T) / height
        inverse.append(np.block([[back.real, -back.imag], [back.imag, back.real]]))
    return jnp.asarray(np.stack(forward), BF16), jnp.asarray(np.stack(inverse), BF16)


def dot(left, right):
    return jnp.dot(left, right, preferred_element_type=F32)


ANY = pl.BlockSpec(memory_space=pltpu.HBM)
SMEM = pl.BlockSpec(memory_space=pltpu.SMEM)
FULL = pl.BlockSpec(memory_space=pltpu.VMEM)


def cost(flops, moved):
    return pl.CostEstimate(flops=flops, bytes_accessed=moved, transcendentals=0)


def params(limit=VMEM_LIMIT):
    return pltpu.CompilerParams(vmem_limit_bytes=limit)


def forward_lanes(load, rows, blocks, lane, twist_ref, left_ref, base=0):
    sub = 16

    def body(i, carry):
        at = pl.ds(pl.multiple_of(i * sub, sub), sub)
        to = pl.ds(pl.multiple_of(i * sub + base, sub), sub)
        real = [load(0, at, b) for b in range(blocks)]
        imag = [load(1, at, b) for b in range(blocks)]
        real, imag = small_dft(real, imag, -1)
        for k in range(blocks):
            if k:
                c, s = twist_ref[0, k : k + 1, :], twist_ref[1, k : k + 1, :]
                re, im = real[k] * c - imag[k] * s, real[k] * s + imag[k] * c
            else:
                re, im = real[k], imag[k]
            left_ref[k, to, 0:lane] = re.astype(BF16)
            left_ref[k, to, lane : 2 * lane] = im.astype(BF16)
        return carry

    lax.fori_loop(0, rows // sub, body, 0)


def slot_products(left_ref, table_ref, me, slot, per_device):
    owner = lax.bitwise_xor(me, slot)
    left = left_ref[pl.ds(owner * per_device, per_device)]
    count, rows, wide = left.shape
    part = dot(left.reshape(count * rows, wide), table_ref[...]).astype(BF16)
    return [part[place * rows : (place + 1) * rows] for place in range(per_device)]


def store_slots(outs, left_ref, table_ref, me, per_device, lane):
    pair = 2 * lane
    span = outs[0].shape[1] // pair
    devices = len(outs) * span // per_device
    for slot in range(devices):
        made = slot_products(left_ref, table_ref, me, slot, per_device)
        for place, part in enumerate(made):
            target = outs[place // span * devices + slot]
            target[:, place % span * pair : (place % span + 1) * pair] = part


def first_kernel(*refs, lane, per_device, chunk, parts):
    field_hbm, twist_hbm, table_hbm, _ = refs[:4]
    outs = refs[4:-5]
    field_ref, left_ref, twist_ref, table_ref, sem = refs[-5:]
    rows, width = field_ref.shape[1], field_ref.shape[2]
    tile = rows // parts
    arriving = [
        pltpu.make_async_copy(
            field_hbm.at[:, pl.ds(chunk * rows + t * tile, tile), :],
            field_ref.at[:, pl.ds(t * tile, tile), :],
            sem.at[t],
        )
        for t in range(parts)
    ]
    twist_in = pltpu.make_async_copy(twist_hbm, twist_ref, sem.at[parts])
    table_in = pltpu.make_async_copy(table_hbm, table_ref, sem.at[parts + 1])
    twist_in.start()
    for copy in arriving:
        copy.start()
    table_in.start()
    twist_in.wait()
    for t in range(parts):
        arriving[t].wait()

        def load(part, at, b, t=t):
            return field_ref[part, pl.ds(at.start + t * tile, at.size), b * lane : (b + 1) * lane]

        forward_lanes(load, tile, width // lane, lane, twist_ref, left_ref, t * tile)
    table_in.wait()
    store_slots(outs, left_ref, table_ref, lax.axis_index("rows"), per_device, lane)


def forward_x(field, tables, lane, devices, chunk, chunks, pieces, after):
    _, rows, width = field.shape
    blocks = width // lane
    per_device = blocks // devices
    rows = rows // chunks
    parts = max(rows // 32, 1)
    shape = jax.ShapeDtypeStruct((rows, per_device * 2 * lane // pieces), BF16)
    made = pl.pallas_call(
        functools.partial(
            first_kernel, lane=lane, per_device=per_device, chunk=chunk, parts=parts
        ),
        in_specs=[ANY, ANY, ANY, pl.BlockSpec(memory_space=pl.ANY)],
        out_specs=[FULL] * (devices * pieces),
        out_shape=[shape] * (devices * pieces),
        scratch_shapes=[
            pltpu.VMEM((2, rows, width), F32),
            pltpu.VMEM((blocks, rows, 2 * lane), BF16),
            pltpu.VMEM(tables[2].shape, F32),
            pltpu.VMEM(tables[0].shape, BF16),
            pltpu.SemaphoreType.DMA((parts + 2,)),
        ],
        compiler_params=params(60 * 1024 * 1024),
        cost_estimate=cost(rows * width * 4000, rows * width * 12),
        name="forward_x",
    )(field, tables[2], tables[0], after)
    return [made[p * devices : (p + 1) * devices] for p in range(pieces)]


def poly(coefficients, t):
    acc = jnp.full_like(t, coefficients[-1])
    for c in coefficients[-2::-1]:
        acc = acc * t + c
    return acc


@functools.lru_cache(maxsize=None)
def wave_series(limit):
    from numpy.polynomial import chebyshev

    nodes = np.cos(np.pi * (np.arange(64) + 0.5) / 64)
    root = np.sqrt((nodes + 1.0) * 0.5 * limit)
    out = []
    for values in (np.cos(root), np.sinc(root / np.pi)):
        fitted = chebyshev.chebfit(nodes, values, 7)
        out.append(tuple(float(c) for c in chebyshev.cheb2poly(fitted)))
    return tuple(out)


def propagator(q, limit):
    root = jnp.sqrt(jnp.abs(q))
    t = q * (2.0 / limit) - 1.0
    cosine, sinc = wave_series(limit)
    upward = q >= 0.0
    t = jnp.where(upward, t, 0.0)
    real = jnp.where(upward, poly(cosine, t), jnp.exp(-root))
    imag = jnp.where(upward, root * poly(sinc, t), 0.0)
    return real, imag


def wave_kernel(me_ref, squared_ref, after_ref, *u_refs, lane, width, height, columns, limit):
    me = me_ref[0]
    depths = squared_ref.shape[0]
    parts = len(u_refs) // depths
    span = columns // parts
    count = height // lane
    blocks = width // lane
    sub = 8
    col = lax.broadcasted_iota(jnp.int32, (sub, lane), 1)
    row_id = lax.broadcasted_iota(jnp.int32, (sub, lane), 0)

    def kappa_squared(index, length):
        signed = jnp.where(2 * index < length, index, index - length)
        kappa = signed.astype(F32) * (2.0 * math.pi / length)
        return kappa * kappa

    def wave_body(i, carry):
        at = pl.multiple_of(i * sub, sub)
        ky2 = [
            kappa_squared(count * (row_id + at) + k, height) for k in range(count // 2 + 1)
        ]
        for c in range(columns):
            kx2 = kappa_squared(blocks * col + me * columns + c, width)
            here = slice(c % span * lane, (c % span + 1) * lane)
            for k in range(count // 2 + 1):
                for depth in range(depths):
                    real, imag = propagator((squared_ref[depth] - ky2[k]) - kx2, limit)
                    u_refs[depth * parts + c // span][k, pl.ds(at, sub), here] = real
                    u_refs[depth * parts + c // span][k, pl.ds(lane + at, sub), here] = imag
        return carry

    lax.fori_loop(0, lane // sub, wave_body, 0)


def waves(me, squared, after, lane, width, height, columns, limit, parts):
    shape = (height // lane // 2 + 1, 2 * lane, columns * lane // parts)
    many = squared.shape[0] * parts
    return pl.pallas_call(
        functools.partial(
            wave_kernel, lane=lane, width=width, height=height, columns=columns, limit=limit
        ),
        in_specs=[SMEM, SMEM, pl.BlockSpec(memory_space=pl.ANY)],
        out_specs=[FULL] * many,
        out_shape=[jax.ShapeDtypeStruct(shape, F32)] * many,
        compiler_params=params(),
        cost_estimate=cost(height * columns * lane * 8000, height * columns * lane * 16),
        name="waves",
    )(me, squared, after)


def xor_permute(values, me):
    values = list(values)
    bit = 1
    while bit < len(values):
        taken = lax.bitwise_and(me, jnp.int32(bit)) != 0
        values = [jnp.where(taken, values[k ^ bit], values[k]) for k in range(len(values))]
        bit *= 2
    return values


def spectral_kernel(*refs, lane, width, devices, chunks, part, parts, tiled):
    me_ref, u_ref, forward_ref, inverse_ref = refs[:4]
    refs = refs[4:]
    total_in = chunks * devices
    ins = [refs[h * devices : (h + 1) * devices] for h in range(chunks)]
    refs = refs[total_in:]
    joins = part == parts - 1 and parts > 1
    if joins:
        priors, refs = refs[:devices], refs[devices:]
    outs = [refs[h * devices : (h + 1) * devices] for h in range(chunks)]
    refs = refs[total_in:]
    x_ref, z_ref, w_ref = refs[:3]
    me = me_ref[0]
    part_rows = ins[0][0].shape[0]
    rows = part_rows * chunks
    height = devices * rows
    count = height // lane
    pair = 2 * lane
    columns = outs[0][0].shape[1] // pair
    sub = 16
    span = columns * pair
    in_base = [part * span] + [0] * (chunks - 1)
    out_base = [0] + [part * span if joins else 0] * (chunks - 1)
    if not tiled:
        in_ref, out_ref, in_sem, out_sem = refs[3:]

        def place_of(slot, h):
            start = lax.bitwise_xor(me, slot) * rows + h * part_rows
            return pl.multiple_of(start, 16)

        def moves(h, slot, inward):
            near = (in_ref if inward else out_ref).at[pl.ds(place_of(slot, h), part_rows), :]
            if inward:
                far = ins[h][slot].at[:, pl.ds(in_base[h], span)]
                return pltpu.make_async_copy(far, near, in_sem.at[h, slot])
            far = outs[h][slot].at[pl.ds(0, part_rows), pl.ds(out_base[h], span)]
            return pltpu.make_async_copy(near, far, out_sem.at[h, slot])

        arriving = [moves(h, k, True) for h in range(chunks) for k in range(devices)]
        for copy in arriving:
            copy.start()
        for copy in arriving:
            copy.wait()
    per_chunk = part_rows // lane

    def fetch(at, base):
        if not tiled:
            return [
                in_ref[pl.ds(pl.multiple_of(at + b * lane, sub), sub), base : base + pair]
                for b in range(count)
            ]
        found = [None] * count
        for h in range(chunks):
            lanes = slice(in_base[h] + base, in_base[h] + base + pair)
            for t in range(per_chunk):
                got = xor_permute(
                    [ref[pl.ds(pl.multiple_of(at + t * lane, sub), sub), lanes] for ref in ins[h]],
                    me,
                )
                for slab in range(devices):
                    found[(slab * chunks + h) * per_chunk + t] = got[slab]
        return found

    def leave(at, base, values):
        if not tiled:
            for b in range(count):
                row = pl.multiple_of(at + b * lane, sub)
                out_ref[pl.ds(row, sub), base : base + pair] = values[b]
            return
        for h in range(chunks):
            lanes = slice(out_base[h] + base, out_base[h] + base + pair)
            for t in range(per_chunk):
                got = xor_permute(
                    [values[(slab * chunks + h) * per_chunk + t] for slab in range(devices)], me
                )
                for slot in range(devices):
                    row = pl.multiple_of(at + t * lane, sub)
                    outs[h][slot][pl.ds(row, sub), lanes] = got[slot]

    for c in range(columns):
        here = slice(c * lane, (c + 1) * lane)

        def load_body(i, carry, c=c, here=here):
            at = pl.multiple_of(i * sub, sub)
            tiles = [tile.astype(F32) for tile in fetch(at, c * pair)]
            real, imag = small_dft(
                [tile[:, :lane] for tile in tiles], [tile[:, lane:] for tile in tiles], -1
            )
            for k in range(count):
                x_ref[k, pl.ds(at, sub), here] = real[k].astype(BF16)
                value = -imag[k] if 2 * k > count else imag[k]
                x_ref[k, pl.ds(lane + at, sub), here] = value.astype(BF16)
            return carry

        lax.fori_loop(0, lane // sub, load_body, 0)

    for k in range(count):
        same = k if 2 * k <= count else count - k
        y = dot(forward_ref[same], x_ref[k])
        yr, yi = y[:lane], y[lane:]
        ur, ui = u_ref[same, 0:lane, :], u_ref[same, lane:pair, :]
        if same == k:
            z_ref[k, 0:lane, :] = (yr * ur - yi * ui).astype(BF16)
            z_ref[k, lane:pair, :] = (yr * ui + yi * ur).astype(BF16)
        else:
            z_ref[k, 0:lane, :] = (yr * ur + yi * ui).astype(BF16)
            z_ref[k, lane:pair, :] = (yi * ur - yr * ui).astype(BF16)
    for k in range(count):
        w_ref[k] = dot(inverse_ref[k if 2 * k <= count else count - k], z_ref[k])

    for c in range(columns):
        here = slice(c * lane, (c + 1) * lane)

        def store_body(i, carry, c=c, here=here):
            at = pl.multiple_of(i * sub, sub)
            real = [w_ref[k, pl.ds(at, sub), here] for k in range(count)]
            imag = [w_ref[k, pl.ds(lane + at, sub), here] for k in range(count)]
            imag = [-im if 2 * k > count else im for k, im in enumerate(imag)]
            real, imag = small_dft(real, imag, 1)
            leave(
                at,
                c * pair,
                [
                    jnp.concatenate([re.astype(BF16), im.astype(BF16)], axis=1)
                    for re, im in zip(real, imag)
                ],
            )
            return carry

        lax.fori_loop(0, lane // sub, store_body, 0)
    if joins:
        for slot in range(devices):
            for h in range(1, chunks):
                outs[h][slot][:, 0 : part * span] = priors[slot][...]
    if not tiled:
        leaving = [moves(h, k, False) for h in range(chunks) for k in range(devices)]
        for copy in leaving:
            copy.start()
        for copy in leaving:
            copy.wait()

    edge = lax.broadcasted_iota(jnp.int32, (EXTRA, span), 0)
    tail = slice(out_base[-1], out_base[-1] + span)
    starts = [outs[0][k][0:EXTRA, :].astype(F32)[0:1] for k in range(devices)]
    ends = [
        outs[-1][k][part_rows - EXTRA : part_rows, tail].astype(F32)[EXTRA - 1 :]
        for k in range(devices)
    ]
    zero = [jnp.zeros((1, span), F32)]
    nexts = xor_permute(xor_permute(starts, me)[1:] + zero, me)
    lasts = xor_permute(zero + xor_permute(ends, me)[:-1], me)
    for k in range(devices):
        after = outs[1][k][0:EXTRA, out_base[1] : out_base[1] + span].astype(F32)[0:1]
        tile = jnp.zeros(edge.shape, F32)
        for row, value in ((0, after), (8, nexts[k]), (EXTRA - 1, lasts[k])):
            tile = jnp.where(edge == row, jnp.broadcast_to(value, edge.shape), tile)
        outs[0][k][part_rows : part_rows + EXTRA, :] = tile.astype(BF16)


def spectral(me, waves, pieces, priors, tables, lane, width, part, parts):
    chunks, devices = len(pieces), len(pieces[0])
    part_rows, wide = pieces[0][0].shape
    rows = part_rows * chunks
    span = wide // parts
    columns = span // (2 * lane)
    height = devices * rows
    count = height // lane
    tiled = part_rows % lane == 0
    joins = part == parts - 1 and parts > 1
    shapes = []
    for h in range(chunks):
        shape = (part_rows, wide if joins else span) if h else (part_rows + EXTRA, span)
        shapes += [jax.ShapeDtypeStruct(shape, BF16)] * devices
    operands = [piece for group in pieces for piece in group]
    if joins:
        operands += priors
    scratch = [
        pltpu.VMEM((count, 2 * lane, columns * lane), BF16),
        pltpu.VMEM((count, 2 * lane, columns * lane), BF16),
        pltpu.VMEM((count, 2 * lane, columns * lane), F32),
    ]
    if not tiled:
        scratch += [pltpu.VMEM((height, span), BF16)] * 2
        scratch += [pltpu.SemaphoreType.DMA((chunks, devices))] * 2
    sent = pl.pallas_call(
        functools.partial(
            spectral_kernel, lane=lane, width=width, devices=devices, chunks=chunks, part=part,
            parts=parts, tiled=tiled,
        ),
        in_specs=[SMEM, FULL, FULL, FULL] + [FULL] * len(operands),
        out_specs=[FULL] * (chunks * devices),
        out_shape=shapes,
        scratch_shapes=scratch,
        compiler_params=params(),
        cost_estimate=cost(height * columns * lane * 8000, height * columns * lane * 16),
        name="spectral",
    )(me, waves, *tables, *operands)
    return [sent[h * devices : (h + 1) * devices] for h in range(chunks)]


def space_kernel(*refs, lane, devices, groups_in, groups_out, chunk, first, last):
    me_ref, factor_ref, coef_hbm, block_hbm, twist_ref, inverse_ref, forward_ref = refs[:7]
    ins = refs[7 : 7 + groups_in * devices]
    at = 7 + groups_in * devices
    if not first:
        carried_ref = refs[at]
        at += 1
    if last and not first:
        at += 1
    outs = refs[at : at + (1 if last else groups_out * devices)]
    at += len(outs)
    kept_ref, sent_ref = refs[at : at + 2]
    at += 2
    if first:
        carry_ref = refs[at]
        at += 1
    (
        coef_ref, block_ref, y_ref, s_ref, left_ref, p_ref, fixed_sem, out_sem,
    ) = refs[at:]
    me = me_ref[0]
    padded, wide = ins[0].shape
    span = wide // (2 * lane)
    per_device = span * groups_in
    rows, width = coef_ref.shape
    blocks = width // lane
    pair = 2 * lane
    coef_copy = pltpu.make_async_copy(
        coef_hbm.at[pl.ds(chunk * rows, rows), :], coef_ref, fixed_sem.at[0]
    )
    block_copy = pltpu.make_async_copy(block_hbm, block_ref, fixed_sem.at[1])
    coef_copy.start()
    block_copy.start()

    for slot in range(devices):
        left = jnp.concatenate(
            [
                ins[place // span * devices + slot][
                    :, place % span * pair : (place % span + 1) * pair
                ]
                for place in range(per_device)
            ],
            axis=0,
        )
        owner = lax.bitwise_xor(me, slot)
        y_ref[pl.ds(owner * per_device, per_device)] = dot(left, inverse_ref[...]).reshape(
            per_device, padded, pair
        )

    def back(start, target):
        real, imag = [], []
        for k in range(blocks):
            re = y_ref[k, pl.ds(start, 8), 0:lane]
            im = y_ref[k, pl.ds(start, 8), lane:pair]
            if k:
                c, s = twist_ref[0, k : k + 1, :], twist_ref[1, k : k + 1, :]
                re, im = re * c + im * s, im * c - re * s
            real.append(re)
            imag.append(im)
        real, imag = small_dft(real, imag, 1)
        for b in range(blocks):
            here = slice(b * lane, (b + 1) * lane)
            s_ref[0, pl.ds(target, 8), here] = real[b]
            s_ref[1, pl.ds(target, 8), here] = imag[b]

    def back_body(i, carry):
        start = pl.multiple_of(i * 8, 8)
        back(start, pl.multiple_of(start + 8, 8))
        return carry

    if first:
        lax.fori_loop(0, rows // 8 + 1, back_body, 0)
        back(rows + 8, 0)
        carry_ref[:, 0:8, :] = s_ref[:, rows : rows + 8, :]
        carry_ref[:, 8:16, :] = s_ref[:, 0:8, :]
    else:
        lax.fori_loop(0, rows // 8, back_body, 0)
        s_ref[:, 0:8, :] = carried_ref[:, 0:8, :]
        s_ref[:, rows + 8 : rows + 16, :] = carried_ref[:, 8:16, :]

    coef_copy.wait()
    gr, gi = factor_ref[0], factor_ref[1]
    sub = 16

    def correct(i, carry, group):
        at = pl.multiple_of(i * sub, sub)
        for b in group:
            here = slice(b * lane, (b + 1) * lane)
            weight = coef_ref[pl.ds(at, sub), here].astype(F32)
            centre, curve = [], []
            for part in range(2):
                near = s_ref[part, pl.ds(at, sub + 16), here]
                mid, up, down = near[8 : 8 + sub], near[9 : 9 + sub], near[7 : 7 + sub]
                centre.append(mid)
                curve.append(up - 2.0 * mid + down)
            re = centre[0] + weight * (gr * curve[0] - gi * curve[1])
            im = centre[1] + weight * (gr * curve[1] + gi * curve[0])
            p_ref[0, pl.ds(at, sub), here] = re
            p_ref[1, pl.ds(at, sub), here] = im
            left_ref[b, pl.ds(at, sub), 0:lane] = re.astype(BF16)
            left_ref[b, pl.ds(at, sub), lane:pair] = im.astype(BF16)
        return carry

    half, _, share = kept_ref.shape
    stride = share // lane
    if stride:
        order = [
            (2 * z + parity) * stride + offset
            for z in range(half) for offset in range(stride) for parity in range(2)
        ]
    else:
        order = list(range(blocks))
    steps = 2 if last and stride and half % 2 == 0 else 1
    leaving = []
    for step in range(steps):
        group = order[step * blocks // steps : (step + 1) * blocks // steps]
        lax.fori_loop(0, rows // sub, functools.partial(correct, group=group), 0)
        if step == 0:
            block_copy.wait()
        even = None
        for b in group:
            here = slice(b * lane, (b + 1) * lane)
            br, bi = block_ref[0, b], block_ref[1, b]
            square = jnp.concatenate(
                [jnp.concatenate([br, bi], axis=1), jnp.concatenate([-bi, br], axis=1)], axis=0
            )
            change = dot(left_ref[b], square)
            re = p_ref[0, :, here] + change[:, 0:lane]
            im = p_ref[1, :, here] + change[:, lane:pair]
            if not stride:
                per_tile = lane // share
                for piece in range(per_tile):
                    owner = b * per_tile + piece
                    value = re[:, piece * share : (piece + 1) * share].astype(BF16)
                    place = lax.bitwise_xor(jnp.int32(owner // 2), me_ref[2])

                    @pl.when(me_ref[1] == owner % 2)
                    def _(place=place, value=value):
                        kept_ref[place] = value

                    @pl.when(me_ref[1] != owner % 2)
                    def _(place=place, value=value):
                        sent_ref[place] = value
            elif (b // stride) % 2 == 0:
                even = re
            else:
                place = lax.bitwise_xor(jnp.int32(b // stride // 2), me_ref[2])
                cols = slice((b % stride) * lane, (b % stride + 1) * lane)
                mine = me_ref[1] == 0
                kept_ref[place, :, cols] = jnp.where(mine, even, re).astype(BF16)
                sent_ref[place, :, cols] = jnp.where(mine, re, even).astype(BF16)
            p_ref[0, :, here] = re
            p_ref[1, :, here] = im
        if last:
            lanes = pl.ds(step * width // steps, width // steps)
            leaving.append(
                pltpu.make_async_copy(
                    p_ref.at[:, :, lanes],
                    outs[0].at[:, pl.ds(chunk * rows, rows), lanes],
                    out_sem.at[step],
                )
            )
            leaving[-1].start()
    if not last:

        def load(part, at, b):
            return p_ref[part, at, b * lane : (b + 1) * lane]

        forward_lanes(load, rows, blocks, lane, twist_ref, left_ref)
        store_slots(outs, left_ref, forward_ref, me, per_device, lane)
    for copy in leaving:
        copy.wait()


def space(me, groups_in, coefficient, factor, inverse_blocks, tables, lane, chunk, carried,
          field, last, groups_out):
    devices = len(groups_in[0])
    pieces = [piece for group in groups_in for piece in group]
    padded, wide = pieces[0].shape
    wide = wide * len(groups_in)
    first = chunk == 0
    rows = padded - EXTRA if first else padded
    all_rows, width = coefficient.shape
    blocks = width // lane
    if last:
        shapes = [jax.ShapeDtypeStruct((2, all_rows, width), F32)]
    else:
        shape = jax.ShapeDtypeStruct((rows, wide // groups_out), BF16)
        shapes = [shape] * (devices * groups_out)
    specs = [ANY if last else FULL] * len(shapes)
    groups = lax.axis_size("freq")
    half = jax.ShapeDtypeStruct((groups // 2, rows, width // groups), BF16)
    shapes = shapes + [half, half]
    specs = specs + [FULL, FULL]
    if first:
        shapes = shapes + [jax.ShapeDtypeStruct((2, 16, width), F32)]
        specs = specs + [FULL]
    operands = [me, factor, coefficient, inverse_blocks, tables[2], tables[1], tables[0], *pieces]
    in_specs = [SMEM, SMEM, ANY, ANY, FULL, FULL, FULL] + [FULL] * len(pieces)
    aliases = {}
    if not first:
        operands.append(carried)
        in_specs.append(FULL)
        if last:
            aliases = {len(operands): 0}
            operands.append(field)
            in_specs.append(ANY)
    got = pl.pallas_call(
        functools.partial(
            space_kernel, lane=lane, devices=devices, groups_in=len(groups_in),
            groups_out=groups_out, chunk=chunk, first=first, last=last,
        ),
        in_specs=in_specs,
        out_specs=specs,
        out_shape=shapes,
        scratch_shapes=[
            pltpu.VMEM((rows, width), BF16),
            pltpu.VMEM(inverse_blocks.shape, BF16),
            pltpu.VMEM((blocks, padded, 2 * lane), F32),
            pltpu.VMEM((2, rows + 16, width), F32),
            pltpu.VMEM((blocks, rows, 2 * lane), BF16),
            pltpu.VMEM((2, rows, width), F32),
            pltpu.SemaphoreType.DMA((2,)),
            pltpu.SemaphoreType.DMA((blocks,)),
        ],
        input_output_aliases=aliases,
        compiler_params=params(),
        cost_estimate=cost(rows * width * 8000, rows * width * 12),
        name="space_last" if last else "space",
    )(*operands)
    got = list(got)
    carry = got.pop() if first else None
    sent, kept = got.pop(), got.pop()
    image = (kept, sent)
    if last:
        return got[0], image, carry
    return [got[p * devices : (p + 1) * devices] for p in range(groups_out)], image, carry


def swap(value, axis, distance):
    count = lax.axis_size(axis)
    return lax.ppermute(value, axis, [(i, i ^ distance) for i in range(count)])


def exchange(pieces):
    return [pieces[0]] + [swap(piece, "rows", k) for k, piece in enumerate(pieces) if k]


def add_all(value, axis, distances):
    return value + sum(swap(value, axis, distance) for distance in distances)


def collect(images):
    joined = []
    for kept, sent in images:
        other = swap(sent, "freq", 1)
        joined.append((kept.astype(F32) + other.astype(F32)).astype(BF16))
    parts = [jnp.concatenate([join[j] for join in joined]) for j in range(joined[0].shape[0])]
    for j in range(1, len(parts)):
        parts[j] = swap(parts[j], "freq", 2 * j)
    return sum(part.astype(F32) for part in parts)


def total(value):
    groups, rows = lax.axis_size("freq"), lax.axis_size("rows")
    value = add_all(value, "freq", [1])
    value = add_all(value, "freq", range(2, groups, 2))
    return add_all(value, "rows", range(1, rows))


def shards(wavefield, block_inverse, coefficient, correction_factor, frequencies, slowness):
    freq_local, rows_local, width = wavefield.shape[1:]
    devices = lax.axis_size("rows")
    height = rows_local * devices
    lane = block_inverse.shape[-1]
    chunks = 2
    limit = (4.5 * 1.0) ** 2 * 1.0001
    x_tables = lane_tables(width, lane)
    y_tables = row_tables(height, lane)
    place = lax.axis_index("freq")
    me = jnp.stack([lax.axis_index("rows"), place % 2, place // 2]).astype(jnp.int32)
    partials = [[None] * chunks for _ in range(DEPTHS)]
    columns = width // lane // devices
    parts = 2 if columns % 2 == 0 else 1
    fields = []
    for f in range(freq_local):
        factor = correction_factor[:, f]
        made, behind = [], slowness
        for h in range(chunks):
            made.append(
                forward_x(
                    wavefield[:, f], x_tables, lane, devices, h, chunks, parts if h else 1, behind
                )
            )
            behind = made[-1][0][0]
        squared = (frequencies[f] * slowness) ** 2
        table = waves(
            me, squared, made[-1][0][0], lane, width, height, columns, limit, parts
        )
        arrived = [[exchange(group) for group in groups] for groups in made]
        for depth_step in range(DEPTHS):
            last = depth_step == DEPTHS - 1
            leaving, priors = [[], []], None
            for p in range(parts):
                sent = spectral(
                    me, table[depth_step * parts + p], [arrived[0][0], arrived[1][p]],
                    priors, y_tables, lane, width, p, parts,
                )
                leaving[0].append(exchange(sent[0]))
                priors = sent[1]
            leaving[1].append(exchange(priors))
            arrived, carry, field = [], None, None
            for h in range(chunks):
                groups_out = parts if h else 1
                made, image, carried = space(
                    me, leaving[h], coefficient, factor, block_inverse[:, f], x_tables, lane,
                    h, carry, field, last, groups_out,
                )
                carry = carry if carried is None else carried
                if last:
                    field = made
                else:
                    arrived.append([exchange(group) for group in made])
                before = partials[depth_step][h]
                if before is not None:
                    image = [
                        (a.astype(F32) + b.astype(F32)).astype(BF16)
                        for a, b in zip(before, image)
                    ]
                partials[depth_step][h] = image
        fields.append(field)
    shares = []
    for d, images in enumerate(partials):
        if d < DEPTHS - 1:
            shares.append(collect(images))
        else:
            shares.append(jnp.concatenate([collect([image]) for image in images]))
    shares = jnp.stack(shares)
    energy = total(jnp.sum(shares * shares, axis=(1, 2)))
    scale = 1.0 / jnp.sqrt(energy / (height * width) + epsilon)
    return shares * scale[:, None, None], jnp.stack(fields, axis=1)


def solution(mesh):
    placed = (
        P(None, "freq", "rows", None),
        P(None, "freq", None, None, None),
        P("rows", None),
        P(None, "freq"),
        P("freq"),
        P(),
    )

    return jax.shard_map(
        shards,
        mesh=mesh,
        in_specs=placed,
        out_specs=(P(None, "rows", "freq"), P(None, "freq", "rows", None)),
        check_vma=False,
    )
```
